32 devices in a mesh: gx: 4 (over y, core), gy: 8 (over z, x).
Axes of the slice: x: 2, y: 2, z: 4, core: 2. Of those that a mesh axis runs over, the one named last changes fastest.
Arguments:
- pixels: int32 [16, 16, 4, 131072], P('gy', 'gx'), may hold values from 0 to 255, as said below
- weights: bfloat16 [16, 16, 4, 131072], P('gy', 'gx'), may hold values from 0.25 to 1
- adjacency: int32 [2, 16, 16], replicated, may hold values 0 or 1
Outputs:
- log_gain: float32 [16, 16], P('gy', 'gx')
The draws below stay inside these ranges and needn't reach their ends.
Inputs may be any that keep to these rules, and one draw needn't show every extreme that they name: `pixels`: bin indices of 8-bit intensities. `adjacency`: entry [0, r, c] is 1 where tile (r, c) and the tile to its right share a usable border, entry [1, r, c] likewise for the tile below; entries of pairs beyond the grid's edge are read by no output.
All inputs are finite; a program needn't handle non-finite values.
Results may differ from the reference program's by a relative error of at most 0.0003.
Values may be sent and summed in bfloat16 or wider, within the bound.
A program may use at most 128 MiB of HBM per device.

```python
import math
import jax
import jax.numpy as jnp
from jax import lax

SEG = 1024
STRIP = 128
ITERS = 20
GR = 16
GC = 16


def draw_pixels(key, part):
    offset_key = jax.random.fold_in(key, 11)
    spread_key = jax.random.fold_in(key, 12)
    jitter_key = jax.random.fold_in(key, 13)
    slope_key = jax.random.fold_in(key, 14)
    length = STRIP * SEG
    column = jnp.arange(GC, dtype=jnp.int32)
    drift = 32 * column // GC
    baseline = drift[None, :] + jax.random.randint(offset_key, (GR, GC), 0, 32, dtype=jnp.int32)
    slope = jax.random.randint(slope_key, (GR, GC, 4, 1), -80, 81, dtype=jnp.int32)
    position = jnp.arange(length, dtype=jnp.int32)[None, None, None, :]
    ramp = 80 + slope * position // length
    spread = jax.random.randint(spread_key, (GR, GC, 4), 20, 61, dtype=jnp.int32)
    jitter = jax.random.randint(jitter_key, (GR, GC, 4, length), 0, spread[..., None], dtype=jnp.int32)
    return jnp.clip(baseline[:, :, None, None] + ramp + jitter, 0, 255).astype(jnp.int32)


def draw_weights(key, part):
    phase_key = jax.random.fold_in(key, 21)
    rough_key = jax.random.fold_in(key, 22)
    length = STRIP * SEG
    along = jnp.arange(length, dtype=jnp.float32) / length
    phase = jax.random.uniform(phase_key, (GR, GC, 4, 1), jnp.float32, -math.pi, math.pi)
    wave = 0.5 + 0.5 * jnp.sin(math.pi * along[None, None, None, :] + phase)
    rough = jax.random.uniform(rough_key, (GR, GC, 4, length), jnp.float32, 0.7, 1.0)
    profile = wave
    return (0.25 + 0.75 * rough * profile).astype(jnp.bfloat16)


def set_ends(array, key, smallest, top_value):
    spot = [jax.random.randint(jax.random.fold_in(key, axis), (), 0, length) for axis, length in enumerate(array.shape)]
    widest = array.shape.index(max(array.shape))
    neighbour = spot[:widest] + [(spot[widest] + 1) % array.shape[widest]] + spot[widest + 1:]
    return array.at[tuple(spot)].set(smallest).at[tuple(neighbour)].set(top_value)


def setup_inputs(seed: int = 0) -> dict:
    arg_keys = jax.random.split(jax.random.key(seed), 4)
    pixels = draw_pixels(jax.random.fold_in(arg_keys[3], 71), 0)
    weights = draw_weights(jax.random.fold_in(arg_keys[3], 71), 0)
    adjacency = set_ends((jax.random.randint(arg_keys[2], (2, GR, GC), 0, 8) < 7).astype(jnp.int32), jax.random.fold_in(arg_keys[2], 1), 0, 1)
    return dict(pixels=pixels, weights=weights, adjacency=adjacency)


anchor_weight = 0.5
mismatch_scale = 8.0


def strip_stats(strip_hist):
    totals = jnp.sum(strip_hist, axis=-1)
    centres = jnp.arange(256, dtype=jnp.float32) + 0.5
    means = jnp.sum(strip_hist * centres, axis=-1) / totals
    cumulative = jnp.cumsum(strip_hist, axis=-1) / totals[..., None]
    return means, cumulative


def pair_terms(own_hist, other_hist, usable):
    own_mean, own_cdf = strip_stats(own_hist)
    other_mean, other_cdf = strip_stats(other_hist)
    distance = jnp.sum(jnp.abs(own_cdf - other_cdf), axis=-1)
    mismatch = (distance - jnp.abs(own_mean - other_mean)) / mismatch_scale
    present = usable > 0
    confidence = jnp.where(present, 1.0 / (0.25 + mismatch * mismatch), 0.0)
    offsets = jnp.where(present, jnp.log(other_mean) - jnp.log(own_mean), 0.0)
    return confidence, offsets


def relax_step(padded, confidence, offsets):
    beside = jnp.stack([padded[:-2, 1:-1], padded[2:, 1:-1], padded[1:-1, :-2], padded[1:-1, 2:]], axis=-1)
    return jnp.sum(confidence * (beside + offsets), axis=-1)


def reference(pixels, weights, adjacency):
    length = pixels.shape[3]

    def row_histogram(row_index):
        own_pixels = lax.dynamic_index_in_dim(pixels, row_index, 0, False)
        own_weights = lax.dynamic_index_in_dim(weights, row_index, 0, False).astype(jnp.float32)
        below_index = jnp.minimum(row_index + 1, GR - 1).astype(jnp.int32)
        above_index = jnp.maximum(row_index - 1, 0).astype(jnp.int32)
        from_below = lax.dynamic_index_in_dim(weights, below_index, 0, False)[:, 0].astype(jnp.float32)
        from_below = from_below * (row_index + 1 < GR).astype(jnp.float32)
        from_above = lax.dynamic_index_in_dim(weights, above_index, 0, False)[:, 1].astype(jnp.float32)
        from_above = from_above * (row_index > 0).astype(jnp.float32)
        zero_strip = jnp.zeros((1, length), jnp.float32)
        from_left = jnp.concatenate([zero_strip, own_weights[:-1, 3]], axis=0)
        from_right = jnp.concatenate([own_weights[1:, 2], zero_strip], axis=0)
        partner = jnp.stack([from_above, from_below, from_left, from_right], axis=1)
        joint_weight = lax.optimization_barrier((own_weights * partner).astype(jnp.bfloat16)).astype(jnp.float32)
        strip_ids = (jnp.arange(GC * 4, dtype=jnp.int32) * 256)[:, None]
        segment = (strip_ids + own_pixels.reshape(GC * 4, length).astype(jnp.int32)).reshape(-1)
        bin_sums = jax.ops.segment_sum(joint_weight.reshape(-1), segment, num_segments=GC * 4 * 256)
        return bin_sums.reshape(GC, 4, 256)

    strip_hist = lax.map(row_histogram, jnp.arange(GR, dtype=jnp.int32))
    zero_row = jnp.zeros((1, GC, 256), jnp.float32)
    zero_column = jnp.zeros((GR, 1, 256), jnp.float32)
    from_above = jnp.concatenate([zero_row, strip_hist[:-1, :, 1]], axis=0)
    from_below = jnp.concatenate([strip_hist[1:, :, 0], zero_row], axis=0)
    from_left = jnp.concatenate([zero_column, strip_hist[:, :-1, 3]], axis=1)
    from_right = jnp.concatenate([strip_hist[:, 1:, 2], zero_column], axis=1)
    partner_hist = jnp.stack([from_above, from_below, from_left, from_right], axis=2)
    across = adjacency[0].astype(jnp.int32)
    downward = adjacency[1].astype(jnp.int32)
    zero_links_row = jnp.zeros((1, GC), jnp.int32)
    zero_links_column = jnp.zeros((GR, 1), jnp.int32)
    up_valid = jnp.concatenate([zero_links_row, downward[:-1]], axis=0)
    down_valid = jnp.concatenate([downward[:-1], zero_links_row], axis=0)
    left_valid = jnp.concatenate([zero_links_column, across[:, :-1]], axis=1)
    right_valid = jnp.concatenate([across[:, :-1], zero_links_column], axis=1)
    usable = jnp.stack([up_valid, down_valid, left_valid, right_valid], axis=-1)
    confidence, offsets = pair_terms(strip_hist, partner_hist, usable)
    denominator = anchor_weight + jnp.sum(confidence, axis=-1)
    log_gain = jnp.zeros((GR, GC), jnp.float32)
    for sweep_index in range(ITERS):
        updated = relax_step(jnp.pad(log_gain, 1), confidence, offsets) / denominator
        log_gain = updated - jnp.sum(updated) / (GR * GC)
    return log_gain
```

```python
import functools
import jax
import jax.numpy as jnp
from jax import lax
from jax.experimental import pallas as pl
from jax.experimental.pallas import tpu as pltpu
from jax.sharding import PartitionSpec as P

ITERS = 20
CHUNKS = 16
LEVELS = 16

anchor_weight = 0.5
mismatch_scale = 8.0


def partner_of(strip):
    row, column, side = strip
    return [
        (row - 1, column, 1),
        (row + 1, column, 0),
        (row, column - 1, 3),
        (row, column + 1, 2),
    ][side]


def border(direction, rows, columns):
    return [
        [(0, column, 0) for column in range(columns)],
        [(rows - 1, column, 1) for column in range(columns)],
        [(row, 0, 2) for row in range(rows)],
        [(row, columns - 1, 3) for row in range(rows)],
    ][direction]


def fold_of(count):
    return max(1, 4 // count)


def roll_rows(values, shift):
    shift = shift % 8
    return values if shift == 0 else pltpu.roll(values, shift, 1)


def wide(values):
    return values.astype(jnp.float32).reshape(values.shape[0] // 8, 8, 128)


def chunk_count(steps):
    count = CHUNKS
    while steps % (count * 16):
        count //= 2
    return count


def strips_kernel(
    shape, chunks, p_ref, w_ref, out_ref,
    p_all, w_all, up_out, down_out, left_out, right_out, up_in, down_in, left_in, right_in, joint, sums,
    p_sem, w_sem, send_sem, recv_sem,
):
    rows, columns, steps = shape
    tiles = [(r, c) for r in range(rows) for c in range(columns)]
    span = steps // chunks
    height = span * 4
    outs = [up_out, down_out, left_out, right_out]
    ins = [up_in, down_in, left_in, right_in]
    x_count, y_count = lax.axis_size("gx"), lax.axis_size("gy")
    x_index, y_index = lax.axis_index("gx"), lax.axis_index("gy")
    present = [y_index > 0, y_index < y_count - 1, x_index > 0, x_index < x_count - 1]
    target = [
        {"gx": x_index, "gy": y_index - 1},
        {"gx": x_index, "gy": y_index + 1},
        {"gx": x_index - 1, "gy": y_index},
        {"gx": x_index + 1, "gy": y_index},
    ]
    borders = [border(d, rows, columns) for d in range(4)]
    folds = [fold_of(len(b)) for b in borders]
    parts = max(folds)

    def chunk(index, size):
        return pl.ds(pl.multiple_of(index * size, 16), size)

    def fetch(index, source, target_ref, sem):
        window = chunk(index, height)
        return pltpu.make_async_copy(
            source.at[:, :, window, :], target_ref.at[:, :, window, :], sem.at[index]
        )

    def send(direction, index):
        window = chunk(index, span * len(borders[direction]))
        opposite = direction ^ 1
        return pltpu.make_async_remote_copy(
            src_ref=outs[direction].at[window, :],
            dst_ref=ins[opposite].at[window, :],
            send_sem=send_sem.at[direction, index],
            recv_sem=recv_sem.at[opposite, index],
            device_id=target[direction],
            device_id_type=pl.DeviceIdType.MESH,
        )

    @pl.loop(0, chunks)
    def _(index):
        fetch(index, w_ref, w_all, w_sem).start()

    @pl.loop(0, chunks)
    def _(index):
        fetch(index, p_ref, p_all, p_sem).start()

    barrier = pltpu.get_barrier_semaphore()
    for direction in range(4):
        @pl.when(present[direction])
        def _():
            pl.semaphore_signal(
                barrier, inc=1, device_id=target[direction], device_id_type=pl.DeviceIdType.MESH
            )

    neighbours = sum(jnp.where(here, 1, 0) for here in present)
    pl.semaphore_wait(barrier, neighbours)

    side = lax.broadcasted_iota(jnp.int32, (1, 8, 128), 1) % 4

    @pl.loop(0, chunks)
    def _(index):
        fetch(index, w_ref, w_all, w_sem).wait()
        for direction in range(4):
            strips, fold = borders[direction], folds[direction]
            for first in range(0, len(strips), 4):
                group = strips[first : first + 4]
                length = height // fold

                @pl.loop(0, length // 16)
                def _(step):
                    total = None
                    for part in range(fold):
                        start = pl.multiple_of(index * height + part * length + step * 16, 16)
                        for number, (row, column, own) in enumerate(group):
                            place = part * len(group) + number
                            value = roll_rows(wide(w_all[row, column, pl.ds(start, 16), :]), place - own)
                            total = value if total is None else jnp.where(side == place, value, total)
                    start = pl.multiple_of(
                        index * span * len(strips) + (first // 4) * height + step * 16, 16
                    )
                    outs[direction][pl.ds(start, 16), :] = total.reshape(16, 128).astype(jnp.bfloat16)

        for direction in range(4):
            @pl.when(present[direction])
            def _():
                send(direction, index).start()

    for direction in range(4):
        @pl.when(jnp.logical_not(present[direction]))
        def _():
            ins[direction][...] = jnp.zeros_like(ins[direction])

    sums[...] = jnp.zeros_like(sums)

    @pl.loop(0, chunks)
    def _(index):
        fetch(index, p_ref, p_all, p_sem).wait()
        for direction in range(4):
            @pl.when(present[direction])
            def _():
                send(direction ^ 1, index).wait_recv()

        length = height // parts
        for part in range(parts):
            @pl.loop(0, length // 16)
            def _(step):
                local = part * length + step * 16
                start = pl.multiple_of(index * height + local, 16)
                values = {tile: wide(w_all[tile[0], tile[1], pl.ds(start, 16), :]) for tile in tiles}

                def facing(tile, own):
                    row, column, other = partner_of((tile[0], tile[1], own))
                    if (row, column) in values:
                        return values[row, column]
                    count, fold = len(borders[own]), folds[own]
                    number = tile[1] if own < 2 else tile[0]
                    piece = part * fold // parts
                    place = piece * count + number if fold > 1 else number % 4
                    offset = pl.multiple_of(
                        index * span * count + (number // 4) * height * (fold == 1)
                        + local - piece * (height // fold), 16
                    )
                    return roll_rows(wide(ins[own][pl.ds(offset, 16), :]), other - place)

                for tile in tiles:
                    from_after = jnp.where(side == 0, facing(tile, 1), facing(tile, 3))
                    from_before = jnp.where(side == 1, facing(tile, 0), facing(tile, 2))
                    partner = jnp.where(side % 2 == 0, roll_rows(from_before, -1), roll_rows(from_after, 1))
                    product = (values[tile] * partner).reshape(16, 128).astype(jnp.bfloat16)
                    joint[tile[0], tile[1], pl.ds(pl.multiple_of(local, 16), 16), :] = product

        for number, (row, column) in enumerate(tiles):
            bins = p_all[row, column, chunk(index, height), :].astype(jnp.int16)
            both = joint[row, column]
            pieces = range(height // 16)
            bins = jnp.concatenate([bins[16 * i : 16 * i + 16] for i in pieces], axis=1)
            both = jnp.concatenate([both[16 * i : 16 * i + 16] for i in pieces], axis=1)
            upper, lower = bins & 240, bins & 15
            zero, one = jnp.zeros_like(both), jnp.ones_like(both)
            left = jnp.concatenate([jnp.where(upper == 16 * i, both, zero) for i in range(LEVELS)], axis=0)
            right = jnp.concatenate([jnp.where(lower == i, one, zero) for i in range(LEVELS)], axis=0)
            sums[number] += lax.dot_general(
                left, right, (((1,), (1,)), ((), ())), preferred_element_type=jnp.float32
            )

    a = lax.broadcasted_iota(jnp.int32, (256, 256), 0)
    b = lax.broadcasted_iota(jnp.int32, (256, 256), 1)
    diagonal = a % 16 == b % 16
    packed = []
    for number in range(len(tiles)):
        kept = jnp.where(diagonal, sums[number], 0.0)
        packed.append(jnp.sum(kept.reshape(16, 16, 256), axis=1))
    packed = jnp.concatenate(packed, axis=0)
    lane = lax.broadcasted_iota(jnp.int32, (256, 64), 0)
    spot = lax.broadcasted_iota(jnp.int32, (256, 64), 1)
    pick = ((lane // 16 == spot % 16) & (lane % 4 == spot // 16)).astype(jnp.float32)
    result = jnp.dot(packed, pick, precision=lax.Precision.HIGHEST, preferred_element_type=jnp.float32)
    for number in range(len(tiles)):
        for own in range(4):
            out_ref[number * 4 + own] = result[number * 16 : number * 16 + 16, own * 16 : own * 16 + 16]

    @pl.loop(0, chunks)
    def _(index):
        for direction in range(4):
            @pl.when(present[direction])
            def _():
                send(direction, index).wait_send()


def strip_sums(pixels, weights):
    rows, columns, sides, length = pixels.shape
    steps = length // 128
    chunks = chunk_count(steps)

    def stacked(array):
        array = array.reshape(rows, columns, sides, steps, 128)
        return array.transpose(0, 1, 3, 2, 4).reshape(rows, columns, steps * sides, 128)

    def halo(count):
        return pltpu.VMEM((steps * count, 128), jnp.bfloat16)

    halos = [halo(columns), halo(columns), halo(rows), halo(rows)]
    return pl.pallas_call(
        functools.partial(strips_kernel, (rows, columns, steps), chunks),
        in_specs=[pl.BlockSpec(memory_space=pl.ANY)] * 2,
        out_specs=pl.BlockSpec(memory_space=pltpu.VMEM),
        out_shape=jax.ShapeDtypeStruct((rows * columns * sides, 16, 16), jnp.float32),
        scratch_shapes=[
            pltpu.VMEM((rows, columns, steps * sides, 128), jnp.int32),
            pltpu.VMEM((rows, columns, steps * sides, 128), jnp.bfloat16),
            *halos,
            *halos,
            pltpu.VMEM((rows, columns, steps * sides // chunks, 128), jnp.bfloat16),
            pltpu.VMEM((rows * columns, 256, 256), jnp.float32),
            pltpu.SemaphoreType.DMA((chunks,)),
            pltpu.SemaphoreType.DMA((chunks,)),
            pltpu.SemaphoreType.DMA((4, chunks)),
            pltpu.SemaphoreType.DMA((4, chunks)),
        ],
        compiler_params=pltpu.CompilerParams(
            collective_id=1, has_side_effects=True, vmem_limit_bytes=60 * 1024 * 1024
        ),
        name="strips",
    )(stacked(pixels), stacked(weights))


def settle_kernel(
    shape, hist_ref, adjacency_ref, out_ref,
    up_row, left_column,
    row_in, column_in, own, other, tile, board, grid,
    near_send, near_recv, far_send, far_recv,
):
    rows, columns = shape
    x_count, y_count = lax.axis_size("gx"), lax.axis_size("gy")
    x_index, y_index = lax.axis_index("gx"), lax.axis_index("gy")
    devices = x_count * y_count
    me = x_index * y_count + y_index
    grid_rows, grid_columns = y_count * rows, x_count * columns
    lanes = grid.shape[1]

    def device(index):
        return {"gx": index // y_count, "gy": index % y_count}

    for column in range(columns):
        up_row[column] = hist_ref[column * 4]
    for row in range(rows):
        left_column[row] = hist_ref[row * columns * 4 + 2]

    barrier = pltpu.get_barrier_semaphore()

    @pl.loop(1, devices)
    def _(step):
        pl.semaphore_signal(
            barrier, inc=1, device_id=device((me + step) % devices), device_id_type=pl.DeviceIdType.MESH
        )

    pl.semaphore_wait(barrier, devices - 1)

    up_copy = pltpu.make_async_remote_copy(
        src_ref=up_row, dst_ref=row_in,
        send_sem=near_send.at[0], recv_sem=near_recv.at[0],
        device_id={"gx": x_index, "gy": (y_index + y_count - 1) % y_count},
        device_id_type=pl.DeviceIdType.MESH,
    )
    left_copy = pltpu.make_async_remote_copy(
        src_ref=left_column, dst_ref=column_in,
        send_sem=near_send.at[1], recv_sem=near_recv.at[1],
        device_id={"gx": (x_index + x_count - 1) % x_count, "gy": y_index},
        device_id_type=pl.DeviceIdType.MESH,
    )
    up_copy.start()
    left_copy.start()

    def local(strip):
        row, column, side = strip
        return hist_ref[(row * columns + column) * 4 + side]

    pairs = [(r, c, 1) for r in range(rows) for c in range(columns)]
    pairs += [(r, c, 3) for r in range(rows) for c in range(columns)]
    late = []
    for number, strip in enumerate(pairs):
        own[number] = local(strip)
        facing_strip = partner_of(strip)
        if facing_strip[0] < rows and facing_strip[1] < columns:
            other[number] = local(facing_strip)
        else:
            late.append((number, strip))
    up_copy.wait()
    left_copy.wait()
    for number, (row, column, side) in late:
        other[number] = row_in[column] if side == 1 else column_in[row]

    count = len(pairs)
    centre = (
        16 * lax.broadcasted_iota(jnp.int32, (count, 16, 16), 1)
        + lax.broadcasted_iota(jnp.int32, (count, 16, 16), 2)
    ).astype(jnp.float32) + 0.5

    def over_bins(values):
        return jnp.sum(jnp.sum(values, axis=1, keepdims=True), axis=2, keepdims=True)

    def share_and_mean(values):
        total = over_bins(values)
        total = jnp.where(total > 0.0, total, 1.0)
        return values / total, over_bins(values * centre) / total

    own_share, own_mean = share_and_mean(own[...])
    other_share, other_mean = share_and_mean(other[...])
    gap = (own_share - other_share).reshape(count * 16, 16)
    low_a = lax.broadcasted_iota(jnp.int32, (16, 16), 0)
    low_b = lax.broadcasted_iota(jnp.int32, (16, 16), 1)
    high_a = lax.broadcasted_iota(jnp.int32, (count * 16, count * 16), 0)
    high_b = lax.broadcasted_iota(jnp.int32, (count * 16, count * 16), 1)
    within = (low_a <= low_b).astype(jnp.float32)
    before = ((high_a // 16 == high_b // 16) & (high_b < high_a)).astype(jnp.float32)
    exact = dict(precision=lax.Precision.HIGHEST, preferred_element_type=jnp.float32)
    running = jnp.dot(gap, within, **exact) + jnp.sum(
        jnp.dot(before, gap, **exact), axis=1, keepdims=True
    )
    distance = over_bins(jnp.abs(running).reshape(count, 16, 16))
    mismatch = (distance - jnp.abs(own_mean - other_mean)) / mismatch_scale
    confidence = (1.0 / (0.25 + mismatch * mismatch)).reshape(count, 1)
    offset = (jnp.log(other_mean) - jnp.log(own_mean)).reshape(count, 1)

    pair = lax.broadcasted_iota(jnp.int32, (count, lanes), 0)
    lane = lax.broadcasted_iota(jnp.int32, (count, lanes), 1)
    direction = pair // (rows * columns)
    pair_row = (pair % (rows * columns)) // columns
    spot = 2 * direction * grid_columns + x_index * columns + pair % columns
    placed = jnp.where(lane == spot, confidence, 0.0) + jnp.where(lane == spot + grid_columns, offset, 0.0)
    for row in range(rows):
        tile[row : row + 1] = jnp.sum(jnp.where(pair_row == row, placed, 0.0), axis=0, keepdims=True)
    board[x_index, y_index] = tile[...]

    def spread(index, source):
        return pltpu.make_async_remote_copy(
            src_ref=tile, dst_ref=board.at[source // y_count, source % y_count],
            send_sem=far_send.at[index], recv_sem=far_recv.at[source],
            device_id=device(index), device_id_type=pl.DeviceIdType.MESH,
        )

    @pl.loop(1, devices)
    def _(step):
        spread((me + step) % devices, me).start()

    @pl.loop(1, devices)
    def _(step):
        source = (me + step) % devices
        spread(source, source).wait_recv()

    for place in range(y_count):
        rows_here = board[0, place]
        for other_x in range(1, x_count):
            rows_here += board[other_x, place]
        grid[place * rows : (place + 1) * rows] = rows_here

    whole = grid[...]
    row_id = lax.broadcasted_iota(jnp.int32, (grid_rows, lanes), 0)
    lane_id = lax.broadcasted_iota(jnp.int32, (grid_rows, lanes), 1)

    def quantity(number, link, keep):
        values = whole if number == 0 else pltpu.roll(whole, lanes - number * grid_columns, 1)
        return jnp.where(keep, values, 0.0)

    def widened(index):
        flat = adjacency_ref[index]
        if lanes > grid_columns:
            blank = jnp.zeros((grid_rows, lanes - grid_columns), jnp.int32)
            flat = jnp.concatenate([flat, blank], axis=1)
        return flat

    keep_down = (widened(1) > 0) & (row_id < grid_rows - 1) & (lane_id < grid_columns)
    keep_right = (widened(0) > 0) & (lane_id < grid_columns - 1)
    down_conf = quantity(0, 1, keep_down)
    down_off = quantity(1, 1, keep_down)
    right_conf = quantity(2, 0, keep_right)
    right_off = quantity(3, 0, keep_right)
    up_conf, up_off = pltpu.roll(down_conf, 1, 0), -pltpu.roll(down_off, 1, 0)
    left_conf, left_off = pltpu.roll(right_conf, 1, 1), -pltpu.roll(right_off, 1, 1)
    confidence_sum = up_conf + down_conf + left_conf + right_conf
    denominator = anchor_weight + confidence_sum
    push = (
        up_conf * up_off + down_conf * down_off + left_conf * left_off + right_conf * right_off
    ) / denominator
    up_part, down_part = up_conf / denominator, down_conf / denominator
    left_part, right_part = left_conf / denominator, right_conf / denominator
    pull = confidence_sum / denominator
    tiles = grid_rows * grid_columns

    def mean_of(values):
        return jnp.sum(jnp.sum(values, axis=0, keepdims=True), axis=1, keepdims=True) / tiles

    def sweep(_, fresh):
        return (
            up_part * pltpu.roll(fresh, 1, 0)
            + down_part * pltpu.roll(fresh, grid_rows - 1, 0)
            + left_part * pltpu.roll(fresh, 1, 1)
            + right_part * pltpu.roll(fresh, lanes - 1, 1)
            + push
        ) - pull * mean_of(fresh)

    fresh = lax.fori_loop(0, ITERS - 1, sweep, push)
    log_gain = fresh - mean_of(fresh)
    result = jnp.zeros((rows, columns), jnp.float32)
    out_row = lax.broadcasted_iota(jnp.int32, (rows, columns), 0)
    out_column = lax.broadcasted_iota(jnp.int32, (rows, columns), 1)
    for row in range(rows):
        line = jnp.sum(jnp.where(row_id == y_index * rows + row, log_gain, 0.0), axis=0, keepdims=True)
        for column in range(columns):
            value = jnp.sum(
                jnp.where(lane_id[:1] == x_index * columns + column, line, 0.0), axis=1, keepdims=True
            )
            result += jnp.where((out_row == row) & (out_column == column), value, 0.0)
    out_ref[...] = result

    @pl.loop(1, devices)
    def _(step):
        spread((me + step) % devices, me).wait_send()


def settle(shape, sums, adjacency):
    rows, columns = shape
    x_count, y_count = lax.axis_size("gx"), lax.axis_size("gy")
    devices = x_count * y_count
    lanes = -(-4 * x_count * columns // 128) * 128
    pairs = 2 * rows * columns
    vmem = pl.BlockSpec(memory_space=pltpu.VMEM)
    return pl.pallas_call(
        functools.partial(settle_kernel, shape),
        in_specs=[vmem] * 2,
        out_specs=vmem,
        out_shape=jax.ShapeDtypeStruct((rows, columns), jnp.float32),
        scratch_shapes=[
            pltpu.VMEM((columns, 16, 16), jnp.float32),
            pltpu.VMEM((rows, 16, 16), jnp.float32),
            pltpu.VMEM((columns, 16, 16), jnp.float32),
            pltpu.VMEM((rows, 16, 16), jnp.float32),
            pltpu.VMEM((pairs, 16, 16), jnp.float32),
            pltpu.VMEM((pairs, 16, 16), jnp.float32),
            pltpu.VMEM((rows, lanes), jnp.float32),
            pltpu.VMEM((x_count, y_count, rows, lanes), jnp.float32),
            pltpu.VMEM((y_count * rows, lanes), jnp.float32),
            pltpu.SemaphoreType.DMA((2,)),
            pltpu.SemaphoreType.DMA((2,)),
            pltpu.SemaphoreType.DMA((devices,)),
            pltpu.SemaphoreType.DMA((devices,)),
        ],
        compiler_params=pltpu.CompilerParams(collective_id=0, has_side_effects=True),
        name="settle",
    )(sums, adjacency)


def body(pixels, weights, adjacency):
    rows, columns = pixels.shape[:2]
    return settle((rows, columns), strip_sums(pixels, weights), adjacency)


def solution(mesh):
    return jax.shard_map(
        body,
        mesh=mesh,
        in_specs=(P("gy", "gx", None, None), P("gy", "gx", None, None), P()),
        out_specs=P("gy", "gx"),
        check_vma=False,
    )
```

```python
import functools
import jax
import jax.numpy as jnp
from jax import lax
from jax.experimental import pallas as pl
from jax.experimental.pallas import tpu as pltpu
from jax.sharding import PartitionSpec as P

ITERS = 20
CHUNKS = 8
LEVELS = 16

anchor_weight = 0.5
mismatch_scale = 8.0


def partner_of(strip):
    row, column, side = strip
    return [
        (row - 1, column, 1),
        (row + 1, column, 0),
        (row, column - 1, 3),
        (row, column + 1, 2),
    ][side]


def border(direction, rows, columns):
    return [
        [(0, column, 0) for column in range(columns)],
        [(rows - 1, column, 1) for column in range(columns)],
        [(row, 0, 2) for row in range(rows)],
        [(row, columns - 1, 3) for row in range(rows)],
    ][direction]


def groups_of(strips):
    groups, first = [], 0
    while first < len(strips):
        size = min(4, len(strips) - first)
        size = 2 if size == 3 else size
        groups.append(strips[first : first + size])
        first += size
    return groups


def inner_groups(rows, columns):
    down = [(row, column, 1) for row in range(rows - 1) for column in range(columns)]
    right = [(row, column, 3) for row in range(rows) for column in range(columns - 1)]
    groups = []
    for strips in groups_of(down) + groups_of(right):
        groups += [strips, [partner_of(strip) for strip in strips]]
    return groups


def all_groups(rows, columns):
    groups = inner_groups(rows, columns)
    for direction in range(4):
        groups += groups_of(border(direction, rows, columns))
    return groups


def roll_rows(values, shift):
    shift = shift % 8
    return values if shift == 0 else pltpu.roll(values, shift, 1)


def gather(read, strips, start, height, side):
    length = height * len(strips) // 4
    total = None
    for place in range(4):
        row, column, own = strips[place % len(strips)]
        value = read[row, column, pl.ds(start + place // len(strips) * length, length), :]
        if value.dtype == jnp.bfloat16:
            value = value.astype(jnp.float32)
        value = roll_rows(value.reshape(length // 8, 8, 128), place - own)
        total = value if total is None else jnp.where(side == place, value, total)
    return total


def flat(values, dtype):
    return values.reshape(values.shape[0] * 8, 128).astype(dtype)


def across(values):
    return jnp.concatenate([values[i : i + 16] for i in range(0, values.shape[0], 16)], axis=1)


def outer_product(bins, joint):
    bins, joint = across(bins), across(joint)
    upper, lower = bins & 240, bins & 15
    zero, one = jnp.zeros_like(joint), jnp.ones_like(joint)
    left = jnp.concatenate([jnp.where(upper == 16 * i, joint, zero) for i in range(LEVELS)], axis=0)
    right = jnp.concatenate([jnp.where(lower == i, one, zero) for i in range(LEVELS)], axis=0)
    return lax.dot_general(left, right, (((1,), (1,)), ((), ())), preferred_element_type=jnp.float32)


def chunk_count(steps):
    count = CHUNKS
    while steps % (count * 16):
        count //= 2
    return count


def strips_kernel(
    shape, chunks, p_ref, w_ref, out_ref,
    p_all, w_all, up_out, down_out, left_out, right_out, up_in, down_in, left_in, right_in, sums,
    p_sem, w_sem, send_sem, recv_sem,
):
    rows, columns, steps = shape
    span = steps // chunks
    height = span * 4
    outs = [up_out, down_out, left_out, right_out]
    ins = [up_in, down_in, left_in, right_in]
    x_count, y_count = lax.axis_size("gx"), lax.axis_size("gy")
    x_index, y_index = lax.axis_index("gx"), lax.axis_index("gy")
    present = [y_index > 0, y_index < y_count - 1, x_index > 0, x_index < x_count - 1]
    target = [
        {"gx": x_index, "gy": y_index - 1},
        {"gx": x_index, "gy": y_index + 1},
        {"gx": x_index - 1, "gy": y_index},
        {"gx": x_index + 1, "gy": y_index},
    ]
    borders = [border(d, rows, columns) for d in range(4)]
    inner = inner_groups(rows, columns)
    groups = all_groups(rows, columns)
    side = lax.broadcasted_iota(jnp.int32, (1, 8, 128), 1) % 4

    def chunk(index, size):
        return pl.ds(pl.multiple_of(index * size, 16), size)

    def fetch(index, source, target_ref, sem):
        window = chunk(index, height)
        return pltpu.make_async_copy(
            source.at[:, :, window, :], target_ref.at[:, :, window, :], sem.at[index]
        )

    def send(direction, index):
        window = chunk(index, span * len(borders[direction]))
        opposite = direction ^ 1
        return pltpu.make_async_remote_copy(
            src_ref=outs[direction].at[window, :],
            dst_ref=ins[opposite].at[window, :],
            send_sem=send_sem.at[direction, index],
            recv_sem=recv_sem.at[opposite, index],
            device_id=target[direction],
            device_id_type=pl.DeviceIdType.MESH,
        )

    def await_halo(direction, index):
        @pl.when(present[direction])
        def _():
            send(direction ^ 1, index).wait_recv()

    @pl.loop(0, chunks)
    def _(index):
        fetch(index, w_ref, w_all, w_sem).start()

    barrier = pltpu.get_barrier_semaphore()
    for direction in range(4):
        @pl.when(present[direction])
        def _():
            pl.semaphore_signal(
                barrier, inc=1, device_id=target[direction], device_id_type=pl.DeviceIdType.MESH
            )

    @pl.loop(0, chunks)
    def _(index):
        fetch(index, p_ref, p_all, p_sem).start()

    neighbours = sum(jnp.where(here, 1, 0) for here in present)
    pl.semaphore_wait(barrier, neighbours)

    @pl.loop(0, chunks)
    def _(index):
        fetch(index, w_ref, w_all, w_sem).wait()
        for direction in range(4):
            base = index * span * len(borders[direction])
            for strips in groups_of(borders[direction]):
                length = height * len(strips) // 4
                total = gather(w_all, strips, pl.multiple_of(index * height, 16), height, side)
                outs[direction][pl.ds(pl.multiple_of(base, 16), length), :] = flat(total, jnp.bfloat16)
                base += length

        for direction in range(4):
            @pl.when(present[direction])
            def _():
                send(direction, index).start()

    for direction in range(4):
        @pl.when(jnp.logical_not(present[direction]))
        def _():
            ins[direction][...] = jnp.zeros_like(ins[direction])

    sums[...] = jnp.zeros_like(sums)

    def bins_of(strips, index):
        return flat(gather(p_all, strips, pl.multiple_of(index * height, 16), height, side), jnp.int16)

    def edge(direction, index):
        base = index * span * len(borders[direction])
        for strips in groups_of(borders[direction]):
            length = height * len(strips) // 4
            window = pl.ds(pl.multiple_of(base, 16), length)
            mine = outs[direction][window, :].astype(jnp.float32)
            joint = (mine * ins[direction][window, :].astype(jnp.float32)).astype(jnp.bfloat16)
            sums[groups.index(strips)] += outer_product(bins_of(strips, index), joint)
            base += length

    @pl.loop(0, chunks)
    def _(index):
        fetch(index, p_ref, p_all, p_sem).wait()
        await_halo(2, index)
        await_halo(3, index)
        for number in range(0, len(inner), 2):
            start = pl.multiple_of(index * height, 16)
            first = gather(w_all, inner[number], start, height, side)
            second = gather(w_all, inner[number + 1], start, height, side)
            joint = flat(first * second, jnp.bfloat16)
            sums[number] += outer_product(bins_of(inner[number], index), joint)
            sums[number + 1] += outer_product(bins_of(inner[number + 1], index), joint)
        edge(2, index)
        edge(3, index)

    @pl.loop(0, chunks)
    def _(index):
        await_halo(0, index)
        await_halo(1, index)
        edge(0, index)
        edge(1, index)

    a = lax.broadcasted_iota(jnp.int32, (256, 256), 0)
    b = lax.broadcasted_iota(jnp.int32, (256, 256), 1)
    diagonal = a % 16 == b % 16
    packed = []
    for number in range(len(groups)):
        kept = jnp.where(diagonal, sums[number], 0.0)
        packed.append(jnp.sum(kept.reshape(16, 16, 256), axis=1))
    packed = jnp.concatenate(packed, axis=0)
    lane = lax.broadcasted_iota(jnp.int32, (256, 64), 0)
    spot = lax.broadcasted_iota(jnp.int32, (256, 64), 1)
    pick = ((lane // 16 == spot % 16) & (lane % 4 == spot // 16)).astype(jnp.float32)
    result = jnp.dot(packed, pick, precision=lax.Precision.HIGHEST, preferred_element_type=jnp.float32)
    for number, strips in enumerate(groups):
        for first, (row, column, own) in enumerate(strips):
            parts = [
                result[number * 16 : number * 16 + 16, place * 16 : place * 16 + 16]
                for place in range(first, 4, len(strips))
            ]
            out_ref[(row * columns + column) * 4 + own] = sum(parts[1:], parts[0])

    @pl.loop(0, chunks)
    def _(index):
        for direction in range(4):
            @pl.when(present[direction])
            def _():
                send(direction, index).wait_send()


def strip_sums(pixels, weights):
    rows, columns, sides, length = pixels.shape
    steps = length // 128
    chunks = chunk_count(steps)

    def stacked(array):
        array = array.reshape(rows, columns, sides, steps, 128)
        return array.transpose(0, 1, 3, 2, 4).reshape(rows, columns, steps * sides, 128)

    def halo(count):
        return pltpu.VMEM((steps * count, 128), jnp.bfloat16)

    halos = [halo(columns), halo(columns), halo(rows), halo(rows)]
    return pl.pallas_call(
        functools.partial(strips_kernel, (rows, columns, steps), chunks),
        in_specs=[pl.BlockSpec(memory_space=pl.ANY)] * 2,
        out_specs=pl.BlockSpec(memory_space=pltpu.VMEM),
        out_shape=jax.ShapeDtypeStruct((rows * columns * sides, 16, 16), jnp.float32),
        scratch_shapes=[
            pltpu.VMEM((rows, columns, steps * sides, 128), jnp.int32),
            pltpu.VMEM((rows, columns, steps * sides, 128), jnp.bfloat16),
            *halos,
            *halos,
            pltpu.VMEM((len(all_groups(rows, columns)), 256, 256), jnp.float32),
            pltpu.SemaphoreType.DMA((chunks,)),
            pltpu.SemaphoreType.DMA((chunks,)),
            pltpu.SemaphoreType.DMA((4, chunks)),
            pltpu.SemaphoreType.DMA((4, chunks)),
        ],
        compiler_params=pltpu.CompilerParams(
            collective_id=1, has_side_effects=True, vmem_limit_bytes=60 * 1024 * 1024
        ),
        name="strips",
    )(stacked(pixels), stacked(weights))


def settle_kernel(
    shape, hist_ref, adjacency_ref, out_ref,
    up_row, left_column,
    row_in, column_in, own, other, tile, board, grid,
    near_send, near_recv, far_send, far_recv,
):
    rows, columns = shape
    x_count, y_count = lax.axis_size("gx"), lax.axis_size("gy")
    x_index, y_index = lax.axis_index("gx"), lax.axis_index("gy")
    devices = x_count * y_count
    me = x_index * y_count + y_index
    grid_rows, grid_columns = y_count * rows, x_count * columns
    lanes = grid.shape[1]

    def device(index):
        return {"gx": index // y_count, "gy": index % y_count}

    for column in range(columns):
        up_row[column] = hist_ref[column * 4]
    for row in range(rows):
        left_column[row] = hist_ref[row * columns * 4 + 2]

    barrier = pltpu.get_barrier_semaphore()

    @pl.loop(1, devices)
    def _(step):
        pl.semaphore_signal(
            barrier, inc=1, device_id=device((me + step) % devices), device_id_type=pl.DeviceIdType.MESH
        )

    pl.semaphore_wait(barrier, devices - 1)

    up_copy = pltpu.make_async_remote_copy(
        src_ref=up_row, dst_ref=row_in,
        send_sem=near_send.at[0], recv_sem=near_recv.at[0],
        device_id={"gx": x_index, "gy": (y_index + y_count - 1) % y_count},
        device_id_type=pl.DeviceIdType.MESH,
    )
    left_copy = pltpu.make_async_remote_copy(
        src_ref=left_column, dst_ref=column_in,
        send_sem=near_send.at[1], recv_sem=near_recv.at[1],
        device_id={"gx": (x_index + x_count - 1) % x_count, "gy": y_index},
        device_id_type=pl.DeviceIdType.MESH,
    )
    up_copy.start()
    left_copy.start()

    def local(strip):
        row, column, side = strip
        return hist_ref[(row * columns + column) * 4 + side]

    pairs = [(r, c, 1) for r in range(rows) for c in range(columns)]
    pairs += [(r, c, 3) for r in range(rows) for c in range(columns)]
    late = []
    for number, strip in enumerate(pairs):
        own[number] = local(strip)
        facing_strip = partner_of(strip)
        if facing_strip[0] < rows and facing_strip[1] < columns:
            other[number] = local(facing_strip)
        else:
            late.append((number, strip))
    up_copy.wait()
    left_copy.wait()
    for number, (row, column, side) in late:
        other[number] = row_in[column] if side == 1 else column_in[row]

    count = len(pairs)
    centre = (
        16 * lax.broadcasted_iota(jnp.int32, (count, 16, 16), 1)
        + lax.broadcasted_iota(jnp.int32, (count, 16, 16), 2)
    ).astype(jnp.float32) + 0.5

    def over_bins(values):
        return jnp.sum(jnp.sum(values, axis=1, keepdims=True), axis=2, keepdims=True)

    def share_and_mean(values):
        total = over_bins(values)
        total = jnp.where(total > 0.0, total, 1.0)
        return values / total, over_bins(values * centre) / total

    own_share, own_mean = share_and_mean(own[...])
    other_share, other_mean = share_and_mean(other[...])
    gap = (own_share - other_share).reshape(count * 16, 16)
    low_a = lax.broadcasted_iota(jnp.int32, (16, 16), 0)
    low_b = lax.broadcasted_iota(jnp.int32, (16, 16), 1)
    high_a = lax.broadcasted_iota(jnp.int32, (count * 16, count * 16), 0)
    high_b = lax.broadcasted_iota(jnp.int32, (count * 16, count * 16), 1)
    within = (low_a <= low_b).astype(jnp.float32)
    before = ((high_a // 16 == high_b // 16) & (high_b < high_a)).astype(jnp.float32)
    exact = dict(precision=lax.Precision.HIGHEST, preferred_element_type=jnp.float32)
    running = jnp.dot(gap, within, **exact) + jnp.sum(
        jnp.dot(before, gap, **exact), axis=1, keepdims=True
    )
    distance = over_bins(jnp.abs(running).reshape(count, 16, 16))
    mismatch = (distance - jnp.abs(own_mean - other_mean)) / mismatch_scale
    confidence = (1.0 / (0.25 + mismatch * mismatch)).reshape(count, 1)
    offset = (jnp.log(other_mean) - jnp.log(own_mean)).reshape(count, 1)

    pair = lax.broadcasted_iota(jnp.int32, (count, lanes), 0)
    lane = lax.broadcasted_iota(jnp.int32, (count, lanes), 1)
    direction = pair // (rows * columns)
    pair_row = (pair % (rows * columns)) // columns
    spot = 2 * direction * grid_columns + x_index * columns + pair % columns
    placed = jnp.where(lane == spot, confidence, 0.0) + jnp.where(lane == spot + grid_columns, offset, 0.0)
    for row in range(rows):
        tile[row : row + 1] = jnp.sum(jnp.where(pair_row == row, placed, 0.0), axis=0, keepdims=True)
    board[x_index, y_index] = tile[...]

    def spread(index, source):
        return pltpu.make_async_remote_copy(
            src_ref=tile, dst_ref=board.at[source // y_count, source % y_count],
            send_sem=far_send.at[index], recv_sem=far_recv.at[source],
            device_id=device(index), device_id_type=pl.DeviceIdType.MESH,
        )

    @pl.loop(1, devices)
    def _(step):
        spread((me + step) % devices, me).start()

    @pl.loop(1, devices)
    def _(step):
        source = (me + step) % devices
        spread(source, source).wait_recv()

    for place in range(y_count):
        rows_here = board[0, place]
        for other_x in range(1, x_count):
            rows_here += board[other_x, place]
        grid[place * rows : (place + 1) * rows] = rows_here

    whole = grid[...]
    row_id = lax.broadcasted_iota(jnp.int32, (grid_rows, lanes), 0)
    lane_id = lax.broadcasted_iota(jnp.int32, (grid_rows, lanes), 1)

    def quantity(number, link, keep):
        values = whole if number == 0 else pltpu.roll(whole, lanes - number * grid_columns, 1)
        return jnp.where(keep, values, 0.0)

    def widened(index):
        flat = adjacency_ref[index]
        if lanes > grid_columns:
            blank = jnp.zeros((grid_rows, lanes - grid_columns), jnp.int32)
            flat = jnp.concatenate([flat, blank], axis=1)
        return flat

    keep_down = (widened(1) > 0) & (row_id < grid_rows - 1) & (lane_id < grid_columns)
    keep_right = (widened(0) > 0) & (lane_id < grid_columns - 1)
    down_conf = quantity(0, 1, keep_down)
    down_off = quantity(1, 1, keep_down)
    right_conf = quantity(2, 0, keep_right)
    right_off = quantity(3, 0, keep_right)
    up_conf, up_off = pltpu.roll(down_conf, 1, 0), -pltpu.roll(down_off, 1, 0)
    left_conf, left_off = pltpu.roll(right_conf, 1, 1), -pltpu.roll(right_off, 1, 1)
    confidence_sum = up_conf + down_conf + left_conf + right_conf
    denominator = anchor_weight + confidence_sum
    push = (
        up_conf * up_off + down_conf * down_off + left_conf * left_off + right_conf * right_off
    ) / denominator
    up_part, down_part = up_conf / denominator, down_conf / denominator
    left_part, right_part = left_conf / denominator, right_conf / denominator
    pull = confidence_sum / denominator
    tiles = grid_rows * grid_columns

    def mean_of(values):
        return jnp.sum(jnp.sum(values, axis=0, keepdims=True), axis=1, keepdims=True) / tiles

    def sweep(_, fresh):
        return (
            up_part * pltpu.roll(fresh, 1, 0)
            + down_part * pltpu.roll(fresh, grid_rows - 1, 0)
            + left_part * pltpu.roll(fresh, 1, 1)
            + right_part * pltpu.roll(fresh, lanes - 1, 1)
            + push
        ) - pull * mean_of(fresh)

    fresh = lax.fori_loop(0, ITERS - 1, sweep, push)
    log_gain = fresh - mean_of(fresh)
    result = jnp.zeros((rows, columns), jnp.float32)
    out_row = lax.broadcasted_iota(jnp.int32, (rows, columns), 0)
    out_column = lax.broadcasted_iota(jnp.int32, (rows, columns), 1)
    for row in range(rows):
        line = jnp.sum(jnp.where(row_id == y_index * rows + row, log_gain, 0.0), axis=0, keepdims=True)
        for column in range(columns):
            value = jnp.sum(
                jnp.where(lane_id[:1] == x_index * columns + column, line, 0.0), axis=1, keepdims=True
            )
            result += jnp.where((out_row == row) & (out_column == column), value, 0.0)
    out_ref[...] = result

    @pl.loop(1, devices)
    def _(step):
        spread((me + step) % devices, me).wait_send()


def settle(shape, sums, adjacency):
    rows, columns = shape
    x_count, y_count = lax.axis_size("gx"), lax.axis_size("gy")
    devices = x_count * y_count
    lanes = -(-4 * x_count * columns // 128) * 128
    pairs = 2 * rows * columns
    vmem = pl.BlockSpec(memory_space=pltpu.VMEM)
    return pl.pallas_call(
        functools.partial(settle_kernel, shape),
        in_specs=[vmem] * 2,
        out_specs=vmem,
        out_shape=jax.ShapeDtypeStruct((rows, columns), jnp.float32),
        scratch_shapes=[
            pltpu.VMEM((columns, 16, 16), jnp.float32),
            pltpu.VMEM((rows, 16, 16), jnp.float32),
            pltpu.VMEM((columns, 16, 16), jnp.float32),
            pltpu.VMEM((rows, 16, 16), jnp.float32),
            pltpu.VMEM((pairs, 16, 16), jnp.float32),
            pltpu.VMEM((pairs, 16, 16), jnp.float32),
            pltpu.VMEM((rows, lanes), jnp.float32),
            pltpu.VMEM((x_count, y_count, rows, lanes), jnp.float32),
            pltpu.VMEM((y_count * rows, lanes), jnp.float32),
            pltpu.SemaphoreType.DMA((2,)),
            pltpu.SemaphoreType.DMA((2,)),
            pltpu.SemaphoreType.DMA((devices,)),
            pltpu.SemaphoreType.DMA((devices,)),
        ],
        compiler_params=pltpu.CompilerParams(collective_id=0, has_side_effects=True),
        name="settle",
    )(sums, adjacency)


def body(pixels, weights, adjacency):
    rows, columns = pixels.shape[:2]
    return settle((rows, columns), strip_sums(pixels, weights), adjacency)


def solution(mesh):
    return jax.shard_map(
        body,
        mesh=mesh,
        in_specs=(P("gy", "gx", None, None), P("gy", "gx", None, None), P()),
        out_specs=P("gy", "gx"),
        check_vma=False,
    )
```

```python
import functools
import jax
import jax.numpy as jnp
from jax import lax
from jax.experimental import pallas as pl
from jax.experimental.pallas import tpu as pltpu
from jax.sharding import PartitionSpec as P

ITERS = 20
CHUNKS = 8
LEVELS = 16

anchor_weight = 0.5
mismatch_scale = 8.0


def partner_of(strip):
    row, column, side = strip
    return [
        (row - 1, column, 1),
        (row + 1, column, 0),
        (row, column - 1, 3),
        (row, column + 1, 2),
    ][side]


def border(direction, rows, columns):
    return [
        [(0, column, 0) for column in range(columns)],
        [(rows - 1, column, 1) for column in range(columns)],
        [(row, 0, 2) for row in range(rows)],
        [(row, columns - 1, 3) for row in range(rows)],
    ][direction]


def groups_of(strips):
    groups, first = [], 0
    while first < len(strips):
        size = min(4, len(strips) - first)
        size = 2 if size == 3 else size
        groups.append(strips[first : first + size])
        first += size
    return groups


def inner_groups(rows, columns):
    down = [(row, column, 1) for row in range(rows - 1) for column in range(columns)]
    right = [(row, column, 3) for row in range(rows) for column in range(columns - 1)]
    groups = []
    for strips in groups_of(down) + groups_of(right):
        groups += [strips, [partner_of(strip) for strip in strips]]
    return groups


def all_groups(rows, columns):
    groups = inner_groups(rows, columns)
    for direction in range(4):
        groups += groups_of(border(direction, rows, columns))
    return groups


def roll_rows(values, shift):
    shift = shift % 8
    return values if shift == 0 else pltpu.roll(values, shift, 1)


def gather(read, strips, start, height, side):
    length = height * len(strips) // 4
    total = None
    for place in range(4):
        row, column, own = strips[place % len(strips)]
        value = read[row, column, pl.ds(start + place // len(strips) * length, length), :]
        if value.dtype == jnp.bfloat16:
            value = value.astype(jnp.float32)
        value = roll_rows(value.reshape(length // 8, 8, 128), place - own)
        total = value if total is None else jnp.where(side == place, value, total)
    return total


def flat(values, dtype):
    return values.reshape(values.shape[0] * 8, 128).astype(dtype)


def across(values):
    return jnp.concatenate([values[i : i + 16] for i in range(0, values.shape[0], 16)], axis=1)


def outer_product(bins, joint):
    bins, joint = across(bins), across(joint)
    upper, lower = bins & 240, bins & 15
    zero, one = jnp.zeros_like(joint), jnp.ones_like(joint)
    left = jnp.concatenate([jnp.where(upper == 16 * i, joint, zero) for i in range(LEVELS)], axis=0)
    right = jnp.concatenate([jnp.where(lower == i, one, zero) for i in range(LEVELS)], axis=0)
    return lax.dot_general(left, right, (((1,), (1,)), ((), ())), preferred_element_type=jnp.float32)


def chunk_count(steps):
    count = CHUNKS
    while steps % (count * 16):
        count //= 2
    return count


def kernel(
    shape, chunks, p_ref, w_ref, adjacency_hbm, out_ref,
    p_all, w_all, up_out, down_out, left_out, right_out, up_in, down_in, left_in, right_in, sums,
    hist, row_out, column_out, row_in, column_in, tile, board, grid, adjacency_ref,
    p_sem, w_sem, send_sem, recv_sem, near_send, near_recv, far_send, far_recv, adjacency_sem,
):
    rows, columns, steps = shape
    span = steps // chunks
    height = span * 4
    outs = [up_out, down_out, left_out, right_out]
    ins = [up_in, down_in, left_in, right_in]
    x_count, y_count = lax.axis_size("gx"), lax.axis_size("gy")
    x_index, y_index = lax.axis_index("gx"), lax.axis_index("gy")
    devices = x_count * y_count
    me = x_index * y_count + y_index
    present = [y_index > 0, y_index < y_count - 1, x_index > 0, x_index < x_count - 1]
    target = [
        {"gx": x_index, "gy": y_index - 1},
        {"gx": x_index, "gy": y_index + 1},
        {"gx": x_index - 1, "gy": y_index},
        {"gx": x_index + 1, "gy": y_index},
    ]
    borders = [border(d, rows, columns) for d in range(4)]
    inner = inner_groups(rows, columns)
    groups = all_groups(rows, columns)
    side = lax.broadcasted_iota(jnp.int32, (1, 8, 128), 1) % 4

    def chunk(index, size):
        return pl.ds(pl.multiple_of(index * size, 16), size)

    def fetch(index, source, target_ref, sem):
        window = chunk(index, height)
        return pltpu.make_async_copy(
            source.at[:, :, window, :], target_ref.at[:, :, window, :], sem.at[index]
        )

    def send(direction, index):
        window = chunk(index, span * len(borders[direction]))
        opposite = direction ^ 1
        return pltpu.make_async_remote_copy(
            src_ref=outs[direction].at[window, :],
            dst_ref=ins[opposite].at[window, :],
            send_sem=send_sem.at[direction],
            recv_sem=recv_sem.at[opposite, index],
            device_id=target[direction],
            device_id_type=pl.DeviceIdType.MESH,
        )

    def await_halo(direction, index):
        @pl.when(present[direction])
        def _():
            send(direction ^ 1, index).wait_recv()

    @pl.loop(0, chunks)
    def _(index):
        fetch(index, w_ref, w_all, w_sem).start()

    barrier = pltpu.get_barrier_semaphore()

    def device(index):
        return {"gx": index // y_count, "gy": index % y_count}

    @pl.loop(1, devices)
    def _(step):
        pl.semaphore_signal(
            barrier, inc=1, device_id=device((me + step) % devices), device_id_type=pl.DeviceIdType.MESH
        )

    def pack(index):
        fetch(index, w_ref, w_all, w_sem).wait()
        for direction in range(4):
            base = index * span * len(borders[direction])
            for strips in groups_of(borders[direction]):
                length = height * len(strips) // 4
                total = gather(w_all, strips, pl.multiple_of(index * height, 16), height, side)
                outs[direction][pl.ds(pl.multiple_of(base, 16), length), :] = flat(total, jnp.bfloat16)
                base += length

    def send_all(index):
        for direction in range(4):
            @pl.when(present[direction])
            def _():
                send(direction, index).start()

    @pl.loop(0, chunks)
    def _(index):
        fetch(index, p_ref, p_all, p_sem).start()

    adjacency_copy = pltpu.make_async_copy(adjacency_hbm, adjacency_ref, adjacency_sem)
    adjacency_copy.start()
    pack(0)
    pl.semaphore_wait(barrier, devices - 1)

    @pl.loop(1, chunks)
    def _(index):
        pack(index)
        send_all(index - 1)

    send_all(chunks - 1)

    for direction in range(4):
        @pl.when(jnp.logical_not(present[direction]))
        def _():
            ins[direction][...] = jnp.zeros_like(ins[direction])

    sums[...] = jnp.zeros_like(sums)

    def bins_of(strips, index):
        return flat(gather(p_all, strips, pl.multiple_of(index * height, 16), height, side), jnp.int16)

    def edge(direction, index):
        base = index * span * len(borders[direction])
        for strips in groups_of(borders[direction]):
            length = height * len(strips) // 4
            window = pl.ds(pl.multiple_of(base, 16), length)
            mine = outs[direction][window, :].astype(jnp.float32)
            joint = (mine * ins[direction][window, :].astype(jnp.float32)).astype(jnp.bfloat16)
            sums[groups.index(strips)] += outer_product(bins_of(strips, index), joint)
            base += length

    @pl.loop(0, chunks)
    def _(index):
        fetch(index, p_ref, p_all, p_sem).wait()
        await_halo(2, index)
        await_halo(3, index)
        for number in range(0, len(inner), 2):
            start = pl.multiple_of(index * height, 16)
            first = gather(w_all, inner[number], start, height, side)
            second = gather(w_all, inner[number + 1], start, height, side)
            joint = flat(first * second, jnp.bfloat16)
            sums[number] += outer_product(bins_of(inner[number], index), joint)
            sums[number + 1] += outer_product(bins_of(inner[number + 1], index), joint)
        edge(2, index)
        edge(3, index)

    near = [
        (row_out, row_in, near_send.at[0], near_recv.at[0], target[0]),
        (column_out, column_in, near_send.at[1], near_recv.at[1], target[2]),
    ]

    def near_copy(number):
        source, destination, send_side, recv_side, where = near[number]
        return pltpu.make_async_remote_copy(
            src_ref=source, dst_ref=destination, send_sem=send_side, recv_sem=recv_side,
            device_id=where, device_id_type=pl.DeviceIdType.MESH,
        )

    def finish(numbers):
        a = lax.broadcasted_iota(jnp.int32, (256, 256), 0)
        b = lax.broadcasted_iota(jnp.int32, (256, 256), 1)
        packed = []
        for number in numbers:
            kept = jnp.where(a % 16 == b % 16, sums[number], 0.0)
            packed.append(jnp.sum(kept.reshape(16, 16, 256), axis=1))
        packed = jnp.concatenate(packed, axis=0)
        lane = lax.broadcasted_iota(jnp.int32, (256, 64), 0)
        spot = lax.broadcasted_iota(jnp.int32, (256, 64), 1)
        pick = ((lane // 16 == spot % 16) & (lane % 4 == spot // 16)).astype(jnp.float32)
        result = jnp.dot(packed, pick, precision=lax.Precision.HIGHEST, preferred_element_type=jnp.float32)
        for order, number in enumerate(numbers):
            strips = groups[number]
            for first, strip in enumerate(strips):
                parts = [
                    result[order * 16 : order * 16 + 16, place * 16 : place * 16 + 16]
                    for place in range(first, 4, len(strips))
                ]
                hist[place_of(strip)] = sum(parts[1:], parts[0])

    def place_of(strip):
        row, column, own = strip
        return (row * columns + column) * 4 + own

    lanes = grid.shape[1]

    def terms(pairs):
        count = len(pairs)
        own = jnp.stack([hist[place_of(strip)] for strip in pairs])
        other = []
        for strip in pairs:
            row, column, _ = partner_of(strip)
            if row == rows:
                other.append(row_in[column])
            elif column == columns:
                other.append(column_in[row])
            else:
                other.append(hist[place_of(partner_of(strip))])
        other = jnp.stack(other)
        centre = (
            16 * lax.broadcasted_iota(jnp.int32, (count, 16, 16), 1)
            + lax.broadcasted_iota(jnp.int32, (count, 16, 16), 2)
        ).astype(jnp.float32) + 0.5

        def over_bins(values):
            return jnp.sum(jnp.sum(values, axis=1, keepdims=True), axis=2, keepdims=True)

        def share_and_mean(values):
            total = over_bins(values)
            total = jnp.where(total > 0.0, total, 1.0)
            return values / total, over_bins(values * centre) / total

        own_share, own_mean = share_and_mean(own)
        other_share, other_mean = share_and_mean(other)
        gap = (own_share - other_share).reshape(count * 16, 16)
        low_a = lax.broadcasted_iota(jnp.int32, (16, 16), 0)
        low_b = lax.broadcasted_iota(jnp.int32, (16, 16), 1)
        high_a = lax.broadcasted_iota(jnp.int32, (count * 16, count * 16), 0)
        high_b = lax.broadcasted_iota(jnp.int32, (count * 16, count * 16), 1)
        within = (low_a <= low_b).astype(jnp.float32)
        before = ((high_a // 16 == high_b // 16) & (high_b < high_a)).astype(jnp.float32)
        exact = dict(precision=lax.Precision.HIGHEST, preferred_element_type=jnp.float32)
        running = jnp.dot(gap, within, **exact) + jnp.sum(
            jnp.dot(before, gap, **exact), axis=1, keepdims=True
        )
        distance = over_bins(jnp.abs(running).reshape(count, 16, 16))
        mismatch = (distance - jnp.abs(own_mean - other_mean)) / mismatch_scale
        confidence = (1.0 / (0.25 + mismatch * mismatch)).reshape(count, 1)
        offset = (jnp.log(other_mean) - jnp.log(own_mean)).reshape(count, 1)
        lane = lax.broadcasted_iota(jnp.int32, (1, lanes), 1)
        lines = [jnp.zeros((1, lanes), jnp.float32) for _ in range(rows)]
        for number, (row, column, own_side) in enumerate(pairs):
            spot = (own_side - 1) * grid_columns + x_index * columns + column
            lines[row] = jnp.where(lane == spot, confidence[number : number + 1], lines[row])
            lines[row] = jnp.where(
                lane == spot + grid_columns, offset[number : number + 1], lines[row]
            )
        return lines

    grid_rows, grid_columns = y_count * rows, x_count * columns
    number_of = {strip: n for n, strips in enumerate(groups) for strip in strips}
    late = sorted({number_of[strip] for strip in borders[0] + borders[1]})
    finish([n for n in range(len(groups)) if n not in late])
    for row in range(rows):
        column_out[row] = hist[place_of((row, 0, 2))]

    @pl.when(present[2])
    def _():
        near_copy(1).start()

    @pl.loop(0, chunks)
    def _(index):
        await_halo(0, index)
        await_halo(1, index)
        edge(0, index)
        edge(1, index)

    finish(late)
    for column in range(columns):
        row_out[column] = hist[place_of((0, column, 0))]

    @pl.when(present[0])
    def _():
        near_copy(0).start()

    @pl.when(present[3])
    def _():
        near_copy(1).wait_recv()

    @pl.when(jnp.logical_not(present[3]))
    def _():
        column_in[...] = jnp.zeros_like(column_in)

    early = [(r, c, 1) for r in range(rows - 1) for c in range(columns)]
    early += [(r, c, 3) for r in range(rows) for c in range(columns)]
    lines = terms(early)

    @pl.when(present[1])
    def _():
        near_copy(0).wait_recv()

    @pl.when(jnp.logical_not(present[1]))
    def _():
        row_in[...] = jnp.zeros_like(row_in)

    more = terms(borders[1])
    for row in range(rows):
        tile[row : row + 1] = lines[row] + more[row]
    board[me] = tile[...]

    def spread(index, source):
        return pltpu.make_async_remote_copy(
            src_ref=tile, dst_ref=board.at[source],
            send_sem=far_send, recv_sem=far_recv,
            device_id=device(index), device_id_type=pl.DeviceIdType.MESH,
        )

    @pl.loop(1, devices)
    def _(step):
        spread((me + step) % devices, me).start()

    for number in range(2):
        @pl.when(present[2 * number])
        def _():
            near_copy(number).wait_send()

    for direction in range(4):
        @pl.when(present[direction])
        def _():
            pltpu.make_async_remote_copy(
                src_ref=outs[direction], dst_ref=ins[direction ^ 1],
                send_sem=send_sem.at[direction], recv_sem=recv_sem.at[direction, 0],
                device_id=target[direction], device_id_type=pl.DeviceIdType.MESH,
            ).wait_send()

    others = pltpu.make_async_remote_copy(
        src_ref=board.at[pl.ds(1, devices - 1)], dst_ref=board.at[pl.ds(1, devices - 1)],
        send_sem=far_send, recv_sem=far_recv,
        device_id=device((me + 1) % devices), device_id_type=pl.DeviceIdType.MESH,
    )
    others.wait_send()
    others.wait_recv()

    for place in range(y_count):
        rows_here = board[place]
        for other_x in range(1, x_count):
            rows_here += board[other_x * y_count + place]
        grid[place * rows : (place + 1) * rows] = rows_here

    adjacency_copy.wait()
    whole = grid[...]
    row_id = lax.broadcasted_iota(jnp.int32, (grid_rows, lanes), 0)
    lane_id = lax.broadcasted_iota(jnp.int32, (grid_rows, lanes), 1)

    def quantity(number, link, keep):
        values = whole if number == 0 else pltpu.roll(whole, lanes - number * grid_columns, 1)
        return jnp.where(keep, values, 0.0)

    def widened(index):
        flat = adjacency_ref[index]
        if lanes > grid_columns:
            blank = jnp.zeros((grid_rows, lanes - grid_columns), jnp.int32)
            flat = jnp.concatenate([flat, blank], axis=1)
        return flat

    keep_down = (widened(1) > 0) & (row_id < grid_rows - 1) & (lane_id < grid_columns)
    keep_right = (widened(0) > 0) & (lane_id < grid_columns - 1)
    down_conf = quantity(0, 1, keep_down)
    down_off = quantity(1, 1, keep_down)
    right_conf = quantity(2, 0, keep_right)
    right_off = quantity(3, 0, keep_right)
    up_conf, up_off = pltpu.roll(down_conf, 1, 0), -pltpu.roll(down_off, 1, 0)
    left_conf, left_off = pltpu.roll(right_conf, 1, 1), -pltpu.roll(right_off, 1, 1)
    confidence_sum = up_conf + down_conf + left_conf + right_conf
    denominator = anchor_weight + confidence_sum
    push = (
        up_conf * up_off + down_conf * down_off + left_conf * left_off + right_conf * right_off
    ) / denominator
    up_part, down_part = up_conf / denominator, down_conf / denominator
    left_part, right_part = left_conf / denominator, right_conf / denominator
    pull = confidence_sum / denominator
    tiles = grid_rows * grid_columns

    def mean_of(values):
        return jnp.sum(jnp.sum(values, axis=0, keepdims=True), axis=1, keepdims=True) / tiles

    def sweep(_, fresh):
        return (
            up_part * pltpu.roll(fresh, 1, 0)
            + down_part * pltpu.roll(fresh, grid_rows - 1, 0)
            + left_part * pltpu.roll(fresh, 1, 1)
            + right_part * pltpu.roll(fresh, lanes - 1, 1)
            + push
        ) - pull * mean_of(fresh)

    fresh = lax.fori_loop(0, ITERS - 1, sweep, push)
    log_gain = fresh - mean_of(fresh)
    result = jnp.zeros((rows, columns), jnp.float32)
    out_row = lax.broadcasted_iota(jnp.int32, (rows, columns), 0)
    out_column = lax.broadcasted_iota(jnp.int32, (rows, columns), 1)
    for row in range(rows):
        line = jnp.sum(jnp.where(row_id == y_index * rows + row, log_gain, 0.0), axis=0, keepdims=True)
        for column in range(columns):
            value = jnp.sum(
                jnp.where(lane_id[:1] == x_index * columns + column, line, 0.0), axis=1, keepdims=True
            )
            result += jnp.where((out_row == row) & (out_column == column), value, 0.0)
    out_ref[...] = result


def body(pixels, weights, adjacency):
    rows, columns, sides, length = pixels.shape
    steps = length // 128
    chunks = chunk_count(steps)
    x_count, y_count = lax.axis_size("gx"), lax.axis_size("gy")
    devices = x_count * y_count
    lanes = -(-4 * x_count * columns // 128) * 128

    def stacked(array):
        array = array.reshape(rows, columns, sides, steps, 128)
        return array.transpose(0, 1, 3, 2, 4).reshape(rows, columns, steps * sides, 128)

    def halo(count):
        return pltpu.VMEM((steps * count, 128), jnp.bfloat16)

    halos = [halo(columns), halo(columns), halo(rows), halo(rows)]
    return pl.pallas_call(
        functools.partial(kernel, (rows, columns, steps), chunks),
        in_specs=[pl.BlockSpec(memory_space=pl.ANY)] * 3,
        out_specs=pl.BlockSpec(memory_space=pltpu.VMEM),
        out_shape=pltpu.VMEM((rows, columns), jnp.float32),
        scratch_shapes=[
            pltpu.VMEM((rows, columns, steps * sides, 128), jnp.int32),
            pltpu.VMEM((rows, columns, steps * sides, 128), jnp.bfloat16),
            *halos,
            *halos,
            pltpu.VMEM((len(all_groups(rows, columns)), 256, 256), jnp.float32),
            pltpu.VMEM((rows * columns * sides, 16, 16), jnp.float32),
            *([pltpu.VMEM((columns, 16, 16), jnp.float32), pltpu.VMEM((rows, 16, 16), jnp.float32)] * 2),
            pltpu.VMEM((rows, lanes), jnp.float32),
            pltpu.VMEM((devices, rows, lanes), jnp.float32),
            pltpu.VMEM((y_count * rows, lanes), jnp.float32),
            pltpu.VMEM(adjacency.shape, jnp.int32),
            pltpu.SemaphoreType.DMA((chunks,)),
            pltpu.SemaphoreType.DMA((chunks,)),
            pltpu.SemaphoreType.DMA((4,)),
            pltpu.SemaphoreType.DMA((4, chunks)),
            pltpu.SemaphoreType.DMA((2,)),
            pltpu.SemaphoreType.DMA((2,)),
            pltpu.SemaphoreType.DMA,
            pltpu.SemaphoreType.DMA,
            pltpu.SemaphoreType.DMA,
        ],
        compiler_params=pltpu.CompilerParams(
            collective_id=0, has_side_effects=True, vmem_limit_bytes=60 * 1024 * 1024
        ),
        name="equalise",
    )(stacked(pixels), stacked(weights), adjacency)


def solution(mesh):
    return jax.shard_map(
        body,
        mesh=mesh,
        in_specs=(P("gy", "gx", None, None), P("gy", "gx", None, None), P()),
        out_specs=P("gy", "gx"),
        check_vma=False,
    )
```

```python
import functools
import jax
import jax.numpy as jnp
from jax import lax
from jax.experimental import pallas as pl
from jax.experimental.pallas import tpu as pltpu
from jax.sharding import PartitionSpec as P

ITERS = 20
CHUNKS = 8
LEVELS = 16

anchor_weight = 0.5
mismatch_scale = 8.0


def partner_of(strip):
    row, column, side = strip
    return [
        (row - 1, column, 1),
        (row + 1, column, 0),
        (row, column - 1, 3),
        (row, column + 1, 2),
    ][side]


def border(direction, rows, columns):
    return [
        [(0, column, 0) for column in range(columns)],
        [(rows - 1, column, 1) for column in range(columns)],
        [(row, 0, 2) for row in range(rows)],
        [(row, columns - 1, 3) for row in range(rows)],
    ][direction]


def groups_of(strips):
    groups, first = [], 0
    while first < len(strips):
        size = min(4, len(strips) - first)
        size = 2 if size == 3 else size
        groups.append(strips[first : first + size])
        first += size
    return groups


def inner_groups(rows, columns):
    down = [(row, column, 1) for row in range(rows - 1) for column in range(columns)]
    right = [(row, column, 3) for row in range(rows) for column in range(columns - 1)]
    groups = []
    for strips in groups_of(down) + groups_of(right):
        groups += [strips, [partner_of(strip) for strip in strips]]
    return groups


def all_groups(rows, columns):
    groups = inner_groups(rows, columns)
    for direction in range(4):
        groups += groups_of(border(direction, rows, columns))
    return groups


def roll_rows(values, shift):
    shift = shift % 8
    return values if shift == 0 else pltpu.roll(values, shift, 1)


def gather(read, strips, start, height, side):
    length = height * len(strips) // 4
    total = None
    for place in range(4):
        row, column, own = strips[place % len(strips)]
        value = read[row, column, pl.ds(start + place // len(strips) * length, length), :]
        if value.dtype == jnp.bfloat16:
            value = value.astype(jnp.float32)
        value = roll_rows(value.reshape(length // 8, 8, 128), place - own)
        total = value if total is None else jnp.where(side == place, value, total)
    return total


def flat(values, dtype):
    return values.reshape(values.shape[0] * 8, 128).astype(dtype)


def across(values):
    return jnp.concatenate([values[i : i + 16] for i in range(0, values.shape[0], 16)], axis=1)


def outer_product(bins, joint):
    bins, joint = across(bins), across(joint)
    upper, lower = bins & 240, bins & 15
    zero, one = jnp.zeros_like(joint), jnp.ones_like(joint)
    left = jnp.concatenate([jnp.where(upper == 16 * i, joint, zero) for i in range(LEVELS)], axis=0)
    right = jnp.concatenate([jnp.where(lower == i, one, zero) for i in range(LEVELS)], axis=0)
    return lax.dot_general(left, right, (((1,), (1,)), ((), ())), preferred_element_type=jnp.float32)


def chunk_count(steps):
    count = CHUNKS
    while steps % (count * 16):
        count //= 2
    return count


def kernel(
    shape, chunks, p_ref, w_ref, adjacency_hbm, out_ref,
    p_all, w_all, up_out, down_out, left_out, right_out, up_in, down_in, left_in, right_in, sums,
    hist, row_out, column_out, row_in, column_in, tile, board, grid, adjacency_ref,
    p_sem, w_sem, send_sem, recv_sem, near_send, near_recv, far_send, far_recv, adjacency_sem,
    relay_in, relay_send, relay_recv,
):
    rows, columns, steps = shape
    span = steps // chunks
    height = span * 4
    outs = [up_out, down_out, left_out, right_out]
    ins = [up_in, down_in, left_in, right_in]
    x_count, y_count = lax.axis_size("gx"), lax.axis_size("gy")
    x_index, y_index = lax.axis_index("gx"), lax.axis_index("gy")
    devices = x_count * y_count
    me = x_index * y_count + y_index
    present = [y_index > 0, y_index < y_count - 1, x_index > 0, x_index < x_count - 1]
    target = [
        {"gx": x_index, "gy": y_index - 1},
        {"gx": x_index, "gy": y_index + 1},
        {"gx": x_index - 1, "gy": y_index},
        {"gx": x_index + 1, "gy": y_index},
    ]
    borders = [border(d, rows, columns) for d in range(4)]
    inner = inner_groups(rows, columns)
    groups = all_groups(rows, columns)
    side = lax.broadcasted_iota(jnp.int32, (1, 8, 128), 1) % 4

    def chunk(index, size):
        return pl.ds(pl.multiple_of(index * size, 16), size)

    def fetch(index, source, target_ref, sem):
        window = chunk(index, height)
        return pltpu.make_async_copy(
            source.at[:, :, window, :], target_ref.at[:, :, window, :], sem.at[index]
        )

    def send(direction, index):
        window = chunk(index, span * len(borders[direction]))
        opposite = direction ^ 1
        return pltpu.make_async_remote_copy(
            src_ref=outs[direction].at[window, :],
            dst_ref=ins[opposite].at[window, :],
            send_sem=send_sem.at[direction],
            recv_sem=recv_sem.at[opposite, index],
            device_id=target[direction],
            device_id_type=pl.DeviceIdType.MESH,
        )

    def await_halo(direction, index):
        @pl.when(present[direction])
        def _():
            send(direction ^ 1, index).wait_recv()

    @pl.loop(0, chunks)
    def _(index):
        fetch(index, w_ref, w_all, w_sem).start()

    barrier = pltpu.get_barrier_semaphore()

    def device(index):
        return {"gx": index // y_count, "gy": index % y_count}

    @pl.loop(1, devices)
    def _(step):
        pl.semaphore_signal(
            barrier, inc=1, device_id=device((me + step) % devices), device_id_type=pl.DeviceIdType.MESH
        )

    def pack(index):
        fetch(index, w_ref, w_all, w_sem).wait()
        for direction in range(4):
            base = index * span * len(borders[direction])
            for strips in groups_of(borders[direction]):
                length = height * len(strips) // 4
                total = gather(w_all, strips, pl.multiple_of(index * height, 16), height, side)
                outs[direction][pl.ds(pl.multiple_of(base, 16), length), :] = flat(total, jnp.bfloat16)
                base += length

    relays = x_count == 4 and y_count % 2 == 0
    layers = y_count // 2
    layer, parity = y_index // 2, y_index % 2
    up_count, down_count = chunks * layer // layers, chunks * (layers - 1 - layer) // layers
    out_count = jnp.where(parity == 1, down_count, up_count)
    relay_count = jnp.where(parity == 1, up_count, down_count)
    relay_chunk = span * columns

    def to_relay(far, index):
        return pltpu.make_async_remote_copy(
            src_ref=outs[far].at[chunk(index, relay_chunk), :],
            dst_ref=relay_in.at[chunk(index, relay_chunk), :],
            send_sem=send_sem.at[far],
            recv_sem=relay_recv.at[index],
            device_id=target[1 - far],
            device_id_type=pl.DeviceIdType.MESH,
        )

    def forward(far, index):
        step = -2 if far == 1 else 2
        return pltpu.make_async_remote_copy(
            src_ref=relay_in.at[chunk(index, relay_chunk), :],
            dst_ref=ins[far].at[chunk(index, relay_chunk), :],
            send_sem=relay_send.at[index],
            recv_sem=recv_sem.at[far, index],
            device_id={"gx": x_index, "gy": y_index + step},
            device_id_type=pl.DeviceIdType.MESH,
        )

    def pass_on(index):
        piece = index - (chunks - relay_count)
        for far in range(2):
            @pl.when((parity == far) & (piece >= 0))
            def _():
                to_relay(far, piece).wait_recv()
                forward(far, piece).start()

    def send_first(index):
        for direction in range(2, 4):
            @pl.when(present[direction])
            def _():
                send(direction, index).start()

        if not relays:
            for direction in range(2):
                @pl.when(present[direction])
                def _():
                    send(direction, index).start()
            return

        for far in range(2):
            @pl.when((parity == far) & present[far] & (index < out_count))
            def _():
                to_relay(far, index).start()

            @pl.when((parity == far) & present[far] & (index >= out_count))
            def _():
                send(far, index).start()

            @pl.when((parity == far) & (out_count == 0))
            def _():
                send(1 - far, index).start()

    def send_rest():
        if not relays:
            return
        for far in range(2):
            @pl.when((parity == far) & (out_count > 0))
            def _():
                @pl.loop(0, chunks)
                def _(index):
                    send(1 - far, index).start()

    @pl.loop(0, chunks)
    def _(index):
        fetch(index, p_ref, p_all, p_sem).start()

    adjacency_copy = pltpu.make_async_copy(adjacency_hbm, adjacency_ref, adjacency_sem)
    adjacency_copy.start()
    pack(0)
    pl.semaphore_wait(barrier, devices - 1)

    @pl.loop(1, chunks)
    def _(index):
        pack(index)
        send_first(index - 1)

    send_first(chunks - 1)
    send_rest()

    for direction in range(4):
        @pl.when(jnp.logical_not(present[direction]))
        def _():
            ins[direction][...] = jnp.zeros_like(ins[direction])

    sums[...] = jnp.zeros_like(sums)

    def bins_of(strips, index):
        return flat(gather(p_all, strips, pl.multiple_of(index * height, 16), height, side), jnp.int16)

    def edge(direction, index):
        base = index * span * len(borders[direction])
        for strips in groups_of(borders[direction]):
            length = height * len(strips) // 4
            window = pl.ds(pl.multiple_of(base, 16), length)
            mine = outs[direction][window, :].astype(jnp.float32)
            joint = (mine * ins[direction][window, :].astype(jnp.float32)).astype(jnp.bfloat16)
            sums[groups.index(strips)] += outer_product(bins_of(strips, index), joint)
            base += length

    @pl.loop(0, chunks)
    def _(index):
        if relays:
            pass_on(index)
        fetch(index, p_ref, p_all, p_sem).wait()
        await_halo(2, index)
        await_halo(3, index)
        for number in range(0, len(inner), 2):
            start = pl.multiple_of(index * height, 16)
            first = gather(w_all, inner[number], start, height, side)
            second = gather(w_all, inner[number + 1], start, height, side)
            joint = flat(first * second, jnp.bfloat16)
            sums[number] += outer_product(bins_of(inner[number], index), joint)
            sums[number + 1] += outer_product(bins_of(inner[number + 1], index), joint)
        edge(2, index)
        edge(3, index)

    near = [
        (row_out, row_in, near_send.at[0], near_recv.at[0], target[0]),
        (column_out, column_in, near_send.at[1], near_recv.at[1], target[2]),
    ]

    def near_copy(number):
        source, destination, send_side, recv_side, where = near[number]
        return pltpu.make_async_remote_copy(
            src_ref=source, dst_ref=destination, send_sem=send_side, recv_sem=recv_side,
            device_id=where, device_id_type=pl.DeviceIdType.MESH,
        )

    def finish(numbers):
        a = lax.broadcasted_iota(jnp.int32, (256, 256), 0)
        b = lax.broadcasted_iota(jnp.int32, (256, 256), 1)
        packed = []
        for number in numbers:
            kept = jnp.where(a % 16 == b % 16, sums[number], 0.0)
            packed.append(jnp.sum(kept.reshape(16, 16, 256), axis=1))
        packed = jnp.concatenate(packed, axis=0)
        lane = lax.broadcasted_iota(jnp.int32, (256, 64), 0)
        spot = lax.broadcasted_iota(jnp.int32, (256, 64), 1)
        pick = ((lane // 16 == spot % 16) & (lane % 4 == spot // 16)).astype(jnp.float32)
        result = jnp.dot(packed, pick, precision=lax.Precision.HIGHEST, preferred_element_type=jnp.float32)
        for order, number in enumerate(numbers):
            strips = groups[number]
            for first, strip in enumerate(strips):
                parts = [
                    result[order * 16 : order * 16 + 16, place * 16 : place * 16 + 16]
                    for place in range(first, 4, len(strips))
                ]
                hist[place_of(strip)] = sum(parts[1:], parts[0])

    def place_of(strip):
        row, column, own = strip
        return (row * columns + column) * 4 + own

    lanes = grid.shape[1]

    def terms(pairs):
        count = len(pairs)
        own = jnp.stack([hist[place_of(strip)] for strip in pairs])
        other = []
        for strip in pairs:
            row, column, _ = partner_of(strip)
            if row == rows:
                other.append(row_in[column])
            elif column == columns:
                other.append(column_in[row])
            else:
                other.append(hist[place_of(partner_of(strip))])
        other = jnp.stack(other)
        centre = (
            16 * lax.broadcasted_iota(jnp.int32, (count, 16, 16), 1)
            + lax.broadcasted_iota(jnp.int32, (count, 16, 16), 2)
        ).astype(jnp.float32) + 0.5

        def over_bins(values):
            return jnp.sum(jnp.sum(values, axis=1, keepdims=True), axis=2, keepdims=True)

        def share_and_mean(values):
            total = over_bins(values)
            total = jnp.where(total > 0.0, total, 1.0)
            return values / total, over_bins(values * centre) / total

        own_share, own_mean = share_and_mean(own)
        other_share, other_mean = share_and_mean(other)
        gap = (own_share - other_share).reshape(count * 16, 16)
        low_a = lax.broadcasted_iota(jnp.int32, (16, 16), 0)
        low_b = lax.broadcasted_iota(jnp.int32, (16, 16), 1)
        high_a = lax.broadcasted_iota(jnp.int32, (count * 16, count * 16), 0)
        high_b = lax.broadcasted_iota(jnp.int32, (count * 16, count * 16), 1)
        within = (low_a <= low_b).astype(jnp.float32)
        before = ((high_a // 16 == high_b // 16) & (high_b < high_a)).astype(jnp.float32)
        exact = dict(precision=lax.Precision.HIGHEST, preferred_element_type=jnp.float32)
        running = jnp.dot(gap, within, **exact) + jnp.sum(
            jnp.dot(before, gap, **exact), axis=1, keepdims=True
        )
        distance = over_bins(jnp.abs(running).reshape(count, 16, 16))
        mismatch = (distance - jnp.abs(own_mean - other_mean)) / mismatch_scale
        confidence = (1.0 / (0.25 + mismatch * mismatch)).reshape(count, 1)
        offset = (jnp.log(other_mean) - jnp.log(own_mean)).reshape(count, 1)
        lane = lax.broadcasted_iota(jnp.int32, (1, lanes), 1)
        lines = [jnp.zeros((1, lanes), jnp.float32) for _ in range(rows)]
        for number, (row, column, own_side) in enumerate(pairs):
            spot = (own_side - 1) * grid_columns + x_index * columns + column
            lines[row] = jnp.where(lane == spot, confidence[number : number + 1], lines[row])
            lines[row] = jnp.where(
                lane == spot + grid_columns, offset[number : number + 1], lines[row]
            )
        return lines

    grid_rows, grid_columns = y_count * rows, x_count * columns
    number_of = {strip: n for n, strips in enumerate(groups) for strip in strips}
    late = sorted({number_of[strip] for strip in borders[0] + borders[1]})
    finish([n for n in range(len(groups)) if n not in late])
    for row in range(rows):
        column_out[row] = hist[place_of((row, 0, 2))]

    @pl.when(present[2])
    def _():
        near_copy(1).start()

    @pl.loop(0, chunks)
    def _(index):
        await_halo(0, index)
        await_halo(1, index)
        edge(0, index)
        edge(1, index)

    finish(late)
    for column in range(columns):
        row_out[column] = hist[place_of((0, column, 0))]

    @pl.when(present[0])
    def _():
        near_copy(0).start()

    @pl.when(present[3])
    def _():
        near_copy(1).wait_recv()

    @pl.when(jnp.logical_not(present[3]))
    def _():
        column_in[...] = jnp.zeros_like(column_in)

    early = [(r, c, 1) for r in range(rows - 1) for c in range(columns)]
    early += [(r, c, 3) for r in range(rows) for c in range(columns)]
    lines = terms(early)

    @pl.when(present[1])
    def _():
        near_copy(0).wait_recv()

    @pl.when(jnp.logical_not(present[1]))
    def _():
        row_in[...] = jnp.zeros_like(row_in)

    more = terms(borders[1])
    for row in range(rows):
        tile[row : row + 1] = lines[row] + more[row]
    board[me] = tile[...]

    def spread(index, source):
        return pltpu.make_async_remote_copy(
            src_ref=tile, dst_ref=board.at[source],
            send_sem=far_send, recv_sem=far_recv,
            device_id=device(index), device_id_type=pl.DeviceIdType.MESH,
        )

    @pl.loop(1, devices)
    def _(step):
        spread((me + step) % devices, me).start()

    for number in range(2):
        @pl.when(present[2 * number])
        def _():
            near_copy(number).wait_send()

    for direction in range(4):
        @pl.when(present[direction])
        def _():
            pltpu.make_async_remote_copy(
                src_ref=outs[direction], dst_ref=ins[direction ^ 1],
                send_sem=send_sem.at[direction], recv_sem=recv_sem.at[direction, 0],
                device_id=target[direction], device_id_type=pl.DeviceIdType.MESH,
            ).wait_send()

    if relays:
        for far in range(2):
            @pl.when(parity == far)
            def _():
                @pl.loop(0, relay_count)
                def _(index):
                    forward(far, index).wait_send()

    others = pltpu.make_async_remote_copy(
        src_ref=board.at[pl.ds(1, devices - 1)], dst_ref=board.at[pl.ds(1, devices - 1)],
        send_sem=far_send, recv_sem=far_recv,
        device_id=device((me + 1) % devices), device_id_type=pl.DeviceIdType.MESH,
    )
    others.wait_send()
    others.wait_recv()

    for place in range(y_count):
        rows_here = board[place]
        for other_x in range(1, x_count):
            rows_here += board[other_x * y_count + place]
        grid[place * rows : (place + 1) * rows] = rows_here

    adjacency_copy.wait()
    whole = grid[...]
    row_id = lax.broadcasted_iota(jnp.int32, (grid_rows, lanes), 0)
    lane_id = lax.broadcasted_iota(jnp.int32, (grid_rows, lanes), 1)

    def quantity(number, link, keep):
        values = whole if number == 0 else pltpu.roll(whole, lanes - number * grid_columns, 1)
        return jnp.where(keep, values, 0.0)

    def widened(index):
        flat = adjacency_ref[index]
        if lanes > grid_columns:
            blank = jnp.zeros((grid_rows, lanes - grid_columns), jnp.int32)
            flat = jnp.concatenate([flat, blank], axis=1)
        return flat

    keep_down = (widened(1) > 0) & (row_id < grid_rows - 1) & (lane_id < grid_columns)
    keep_right = (widened(0) > 0) & (lane_id < grid_columns - 1)
    down_conf = quantity(0, 1, keep_down)
    down_off = quantity(1, 1, keep_down)
    right_conf = quantity(2, 0, keep_right)
    right_off = quantity(3, 0, keep_right)
    up_conf, up_off = pltpu.roll(down_conf, 1, 0), -pltpu.roll(down_off, 1, 0)
    left_conf, left_off = pltpu.roll(right_conf, 1, 1), -pltpu.roll(right_off, 1, 1)
    confidence_sum = up_conf + down_conf + left_conf + right_conf
    denominator = anchor_weight + confidence_sum
    push = (
        up_conf * up_off + down_conf * down_off + left_conf * left_off + right_conf * right_off
    ) / denominator
    up_part, down_part = up_conf / denominator, down_conf / denominator
    left_part, right_part = left_conf / denominator, right_conf / denominator
    pull = confidence_sum / denominator
    tiles = grid_rows * grid_columns

    def mean_of(values):
        return jnp.sum(jnp.sum(values, axis=0, keepdims=True), axis=1, keepdims=True) / tiles

    def sweep(_, fresh):
        return (
            up_part * pltpu.roll(fresh, 1, 0)
            + down_part * pltpu.roll(fresh, grid_rows - 1, 0)
            + left_part * pltpu.roll(fresh, 1, 1)
            + right_part * pltpu.roll(fresh, lanes - 1, 1)
            + push
        ) - pull * mean_of(fresh)

    fresh = lax.fori_loop(0, ITERS - 1, sweep, push)
    log_gain = fresh - mean_of(fresh)
    result = jnp.zeros((rows, columns), jnp.float32)
    out_row = lax.broadcasted_iota(jnp.int32, (rows, columns), 0)
    out_column = lax.broadcasted_iota(jnp.int32, (rows, columns), 1)
    for row in range(rows):
        line = jnp.sum(jnp.where(row_id == y_index * rows + row, log_gain, 0.0), axis=0, keepdims=True)
        for column in range(columns):
            value = jnp.sum(
                jnp.where(lane_id[:1] == x_index * columns + column, line, 0.0), axis=1, keepdims=True
            )
            result += jnp.where((out_row == row) & (out_column == column), value, 0.0)
    out_ref[...] = result


def body(pixels, weights, adjacency):
    rows, columns, sides, length = pixels.shape
    steps = length // 128
    chunks = chunk_count(steps)
    x_count, y_count = lax.axis_size("gx"), lax.axis_size("gy")
    devices = x_count * y_count
    lanes = -(-4 * x_count * columns // 128) * 128

    def stacked(array):
        array = array.reshape(rows, columns, sides, steps, 128)
        return array.transpose(0, 1, 3, 2, 4).reshape(rows, columns, steps * sides, 128)

    def halo(count):
        return pltpu.VMEM((steps * count, 128), jnp.bfloat16)

    halos = [halo(columns), halo(columns), halo(rows), halo(rows)]
    return pl.pallas_call(
        functools.partial(kernel, (rows, columns, steps), chunks),
        in_specs=[pl.BlockSpec(memory_space=pl.ANY)] * 3,
        out_specs=pl.BlockSpec(memory_space=pltpu.VMEM),
        out_shape=pltpu.VMEM((rows, columns), jnp.float32),
        scratch_shapes=[
            pltpu.VMEM((rows, columns, steps * sides, 128), jnp.int32),
            pltpu.VMEM((rows, columns, steps * sides, 128), jnp.bfloat16),
            *halos,
            *halos,
            pltpu.VMEM((len(all_groups(rows, columns)), 256, 256), jnp.float32),
            pltpu.VMEM((rows * columns * sides, 16, 16), jnp.float32),
            *([pltpu.VMEM((columns, 16, 16), jnp.float32), pltpu.VMEM((rows, 16, 16), jnp.float32)] * 2),
            pltpu.VMEM((rows, lanes), jnp.float32),
            pltpu.VMEM((devices, rows, lanes), jnp.float32),
            pltpu.VMEM((y_count * rows, lanes), jnp.float32),
            pltpu.VMEM(adjacency.shape, jnp.int32),
            pltpu.SemaphoreType.DMA((chunks,)),
            pltpu.SemaphoreType.DMA((chunks,)),
            pltpu.SemaphoreType.DMA((4,)),
            pltpu.SemaphoreType.DMA((4, chunks)),
            pltpu.SemaphoreType.DMA((2,)),
            pltpu.SemaphoreType.DMA((2,)),
            pltpu.SemaphoreType.DMA,
            pltpu.SemaphoreType.DMA,
            pltpu.SemaphoreType.DMA,
            halo(columns),
            pltpu.SemaphoreType.DMA((chunks,)),
            pltpu.SemaphoreType.DMA((chunks,)),
        ],
        compiler_params=pltpu.CompilerParams(
            collective_id=0, has_side_effects=True, vmem_limit_bytes=60 * 1024 * 1024
        ),
        name="equalise",
    )(stacked(pixels), stacked(weights), adjacency)


def solution(mesh):
    return jax.shard_map(
        body,
        mesh=mesh,
        in_specs=(P("gy", "gx", None, None), P("gy", "gx", None, None), P()),
        out_specs=P("gy", "gx"),
        check_vma=False,
    )
```

```python
import functools
import jax
import jax.numpy as jnp
from jax import lax
from jax.experimental import pallas as pl
from jax.experimental.pallas import tpu as pltpu
from jax.sharding import PartitionSpec as P

ITERS = 20
CHUNKS = 8
LEVELS = 16

anchor_weight = 0.5
mismatch_scale = 8.0


def partner_of(strip):
    row, column, side = strip
    return [
        (row - 1, column, 1),
        (row + 1, column, 0),
        (row, column - 1, 3),
        (row, column + 1, 2),
    ][side]


def border(direction, rows, columns):
    return [
        [(0, column, 0) for column in range(columns)],
        [(rows - 1, column, 1) for column in range(columns)],
        [(row, 0, 2) for row in range(rows)],
        [(row, columns - 1, 3) for row in range(rows)],
    ][direction]


def groups_of(strips):
    groups, first = [], 0
    while first < len(strips):
        size = min(4, len(strips) - first)
        size = 2 if size == 3 else size
        groups.append(strips[first : first + size])
        first += size
    return groups


def inner_groups(rows, columns):
    down = [(row, column, 1) for row in range(rows - 1) for column in range(columns)]
    right = [(row, column, 3) for row in range(rows) for column in range(columns - 1)]
    groups = []
    for strips in groups_of(down) + groups_of(right):
        groups += [strips, [partner_of(strip) for strip in strips]]
    return groups


def all_groups(rows, columns):
    groups = inner_groups(rows, columns)
    for direction in range(4):
        groups += groups_of(border(direction, rows, columns))
    return groups


def roll_rows(values, shift):
    shift = shift % 8
    return values if shift == 0 else pltpu.roll(values, shift, 1)


def gather(read, strips, start, height, side):
    length = height * len(strips) // 4
    total = None
    for place in range(4):
        row, column, own = strips[place % len(strips)]
        value = read[row, column, pl.ds(start + place // len(strips) * length, length), :]
        if value.dtype == jnp.bfloat16:
            value = value.astype(jnp.float32)
        value = roll_rows(value.reshape(length // 8, 8, 128), place - own)
        total = value if total is None else jnp.where(side == place, value, total)
    return total


def flat(values, dtype):
    return values.reshape(values.shape[0] * 8, 128).astype(dtype)


def across(values):
    return jnp.concatenate([values[i : i + 16] for i in range(0, values.shape[0], 16)], axis=1)


def outer_product(bins, joint):
    bins, joint = across(bins), across(joint)
    upper, lower = bins & 240, bins & 15
    zero, one = jnp.zeros_like(joint), jnp.ones_like(joint)
    left = jnp.concatenate([jnp.where(upper == 16 * i, joint, zero) for i in range(LEVELS)], axis=0)
    right = jnp.concatenate([jnp.where(lower == i, one, zero) for i in range(LEVELS)], axis=0)
    return lax.dot_general(left, right, (((1,), (1,)), ((), ())), preferred_element_type=jnp.float32)


def chunk_count(steps):
    count = CHUNKS
    while steps % (count * 16):
        count //= 2
    return count


def kernel(
    shape, chunks, p_ref, w_ref, adjacency_hbm, out_ref,
    p_all, w_all, up_out, down_out, left_out, right_out, up_in, down_in, left_in, right_in, sums,
    hist, row_out, column_out, row_in, column_in, tile, board, grid, adjacency_ref,
    p_sem, w_sem, send_sem, recv_sem, near_send, near_recv, far_send, far_recv, adjacency_sem,
    relay_in, relay_send, relay_recv, told,
):
    rows, columns, steps = shape
    span = steps // chunks
    height = span * 4
    outs = [up_out, down_out, left_out, right_out]
    ins = [up_in, down_in, left_in, right_in]
    x_count, y_count = lax.axis_size("gx"), lax.axis_size("gy")
    x_index, y_index = lax.axis_index("gx"), lax.axis_index("gy")
    devices = x_count * y_count
    me = x_index * y_count + y_index
    present = [y_index > 0, y_index < y_count - 1, x_index > 0, x_index < x_count - 1]
    target = [
        {"gx": x_index, "gy": y_index - 1},
        {"gx": x_index, "gy": y_index + 1},
        {"gx": x_index - 1, "gy": y_index},
        {"gx": x_index + 1, "gy": y_index},
    ]
    borders = [border(d, rows, columns) for d in range(4)]
    inner = inner_groups(rows, columns)
    groups = all_groups(rows, columns)
    side = lax.broadcasted_iota(jnp.int32, (1, 8, 128), 1) % 4

    def chunk(index, size):
        return pl.ds(pl.multiple_of(index * size, 16), size)

    def fetch(index, source, target_ref, sem):
        window = chunk(index, height)
        return pltpu.make_async_copy(
            source.at[:, :, window, :], target_ref.at[:, :, window, :], sem.at[index]
        )

    def send(direction, index):
        window = chunk(index, span * len(borders[direction]))
        opposite = direction ^ 1
        return pltpu.make_async_remote_copy(
            src_ref=outs[direction].at[window, :],
            dst_ref=ins[opposite].at[window, :],
            send_sem=send_sem.at[direction],
            recv_sem=recv_sem.at[opposite, index],
            device_id=target[direction],
            device_id_type=pl.DeviceIdType.MESH,
        )

    def await_halo(direction, index):
        @pl.when(present[direction])
        def _():
            send(direction ^ 1, index).wait_recv()

    @pl.loop(0, chunks)
    def _(index):
        fetch(index, w_ref, w_all, w_sem).start()

    barrier = pltpu.get_barrier_semaphore()

    def device(index):
        return {"gx": index // y_count, "gy": index % y_count}

    greeted = list(zip(present, target))
    greeted.append((y_index > 1, {"gx": x_index, "gy": y_index - 2}))
    greeted.append((y_index < y_count - 2, {"gx": x_index, "gy": y_index + 2}))
    for here, there in greeted:
        @pl.when(here)
        def _():
            pl.semaphore_signal(barrier, inc=1, device_id=there, device_id_type=pl.DeviceIdType.MESH)

    rounds = -(-(x_count + y_count - 4) // chunks)

    def tell():
        for direction in range(4):
            @pl.when(present[direction])
            def _():
                pl.semaphore_signal(
                    told.at[direction ^ 1], inc=1, device_id=target[direction],
                    device_id_type=pl.DeviceIdType.MESH,
                )

    def hear():
        for direction in range(4):
            @pl.when(present[direction])
            def _():
                pl.semaphore_wait(told.at[direction], 1)

    def pass_word():
        for _ in range(rounds):
            hear()
            tell()

    def pack(index):
        fetch(index, w_ref, w_all, w_sem).wait()
        for direction in range(4):
            base = index * span * len(borders[direction])
            for strips in groups_of(borders[direction]):
                length = height * len(strips) // 4
                total = gather(w_all, strips, pl.multiple_of(index * height, 16), height, side)
                outs[direction][pl.ds(pl.multiple_of(base, 16), length), :] = flat(total, jnp.bfloat16)
                base += length

    relays = x_count == 4 and y_count % 2 == 0
    layers = y_count // 2
    layer, parity = y_index // 2, y_index % 2
    up_count, down_count = chunks * layer // layers, chunks * (layers - 1 - layer) // layers
    out_count = jnp.where(parity == 1, down_count, up_count)
    relay_count = jnp.where(parity == 1, up_count, down_count)
    relay_chunk = span * columns

    def to_relay(far, index):
        return pltpu.make_async_remote_copy(
            src_ref=outs[far].at[chunk(index, relay_chunk), :],
            dst_ref=relay_in.at[chunk(index, relay_chunk), :],
            send_sem=send_sem.at[far],
            recv_sem=relay_recv.at[index],
            device_id=target[1 - far],
            device_id_type=pl.DeviceIdType.MESH,
        )

    def forward(far, index):
        step = -2 if far == 1 else 2
        return pltpu.make_async_remote_copy(
            src_ref=relay_in.at[chunk(index, relay_chunk), :],
            dst_ref=ins[far].at[chunk(index, relay_chunk), :],
            send_sem=relay_send.at[index],
            recv_sem=recv_sem.at[far, index],
            device_id={"gx": x_index, "gy": y_index + step},
            device_id_type=pl.DeviceIdType.MESH,
        )

    def pass_on(index):
        piece = index - (chunks - relay_count)
        for far in range(2):
            @pl.when((parity == far) & (piece >= 0))
            def _():
                to_relay(far, piece).wait_recv()
                forward(far, piece).start()

    def send_first(index):
        for direction in range(2, 4):
            @pl.when(present[direction])
            def _():
                send(direction, index).start()

        if not relays:
            for direction in range(2):
                @pl.when(present[direction])
                def _():
                    send(direction, index).start()
            return

        for far in range(2):
            @pl.when((parity == far) & present[far] & (index < out_count))
            def _():
                to_relay(far, index).start()

            @pl.when((parity == far) & present[far] & (index >= out_count))
            def _():
                send(far, index).start()

            @pl.when((parity == far) & (out_count == 0))
            def _():
                send(1 - far, index).start()

    def send_rest():
        if not relays:
            return
        for far in range(2):
            @pl.when((parity == far) & (out_count > 0))
            def _():
                @pl.loop(0, chunks)
                def _(index):
                    send(1 - far, index).start()

    @pl.loop(0, chunks)
    def _(index):
        fetch(index, p_ref, p_all, p_sem).start()

    adjacency_copy = pltpu.make_async_copy(adjacency_hbm, adjacency_ref, adjacency_sem)
    adjacency_copy.start()
    pack(0)
    pl.semaphore_wait(barrier, sum(jnp.where(here, 1, 0) for here, _ in greeted))
    tell()

    @pl.loop(1, chunks)
    def _(index):
        pack(index)
        send_first(index - 1)

    send_first(chunks - 1)
    send_rest()

    for direction in range(4):
        @pl.when(jnp.logical_not(present[direction]))
        def _():
            ins[direction][...] = jnp.zeros_like(ins[direction])

    sums[...] = jnp.zeros_like(sums)

    def bins_of(strips, index):
        return flat(gather(p_all, strips, pl.multiple_of(index * height, 16), height, side), jnp.int16)

    def edge(direction, index):
        base = index * span * len(borders[direction])
        for strips in groups_of(borders[direction]):
            length = height * len(strips) // 4
            window = pl.ds(pl.multiple_of(base, 16), length)
            mine = outs[direction][window, :].astype(jnp.float32)
            joint = (mine * ins[direction][window, :].astype(jnp.float32)).astype(jnp.bfloat16)
            sums[groups.index(strips)] += outer_product(bins_of(strips, index), joint)
            base += length

    @pl.loop(0, chunks)
    def _(index):
        pass_word()
        if relays:
            pass_on(index)
        fetch(index, p_ref, p_all, p_sem).wait()
        await_halo(2, index)
        await_halo(3, index)
        for number in range(0, len(inner), 2):
            start = pl.multiple_of(index * height, 16)
            first = gather(w_all, inner[number], start, height, side)
            second = gather(w_all, inner[number + 1], start, height, side)
            joint = flat(first * second, jnp.bfloat16)
            sums[number] += outer_product(bins_of(inner[number], index), joint)
            sums[number + 1] += outer_product(bins_of(inner[number + 1], index), joint)
        edge(2, index)
        edge(3, index)

    near = [
        (row_out, row_in, near_send.at[0], near_recv.at[0], target[0]),
        (column_out, column_in, near_send.at[1], near_recv.at[1], target[2]),
    ]

    def near_copy(number):
        source, destination, send_side, recv_side, where = near[number]
        return pltpu.make_async_remote_copy(
            src_ref=source, dst_ref=destination, send_sem=send_side, recv_sem=recv_side,
            device_id=where, device_id_type=pl.DeviceIdType.MESH,
        )

    def finish(numbers):
        a = lax.broadcasted_iota(jnp.int32, (256, 256), 0)
        b = lax.broadcasted_iota(jnp.int32, (256, 256), 1)
        packed = []
        for number in numbers:
            kept = jnp.where(a % 16 == b % 16, sums[number], 0.0)
            packed.append(jnp.sum(kept.reshape(16, 16, 256), axis=1))
        packed = jnp.concatenate(packed, axis=0)
        lane = lax.broadcasted_iota(jnp.int32, (256, 64), 0)
        spot = lax.broadcasted_iota(jnp.int32, (256, 64), 1)
        pick = ((lane // 16 == spot % 16) & (lane % 4 == spot // 16)).astype(jnp.float32)
        result = jnp.dot(packed, pick, precision=lax.Precision.HIGHEST, preferred_element_type=jnp.float32)
        for order, number in enumerate(numbers):
            strips = groups[number]
            for first, strip in enumerate(strips):
                parts = [
                    result[order * 16 : order * 16 + 16, place * 16 : place * 16 + 16]
                    for place in range(first, 4, len(strips))
                ]
                hist[place_of(strip)] = sum(parts[1:], parts[0])

    def place_of(strip):
        row, column, own = strip
        return (row * columns + column) * 4 + own

    lanes = grid.shape[1]

    def terms(pairs):
        count = len(pairs)
        own = jnp.stack([hist[place_of(strip)] for strip in pairs])
        other = []
        for strip in pairs:
            row, column, _ = partner_of(strip)
            if row == rows:
                other.append(row_in[column])
            elif column == columns:
                other.append(column_in[row])
            else:
                other.append(hist[place_of(partner_of(strip))])
        other = jnp.stack(other)
        centre = (
            16 * lax.broadcasted_iota(jnp.int32, (count, 16, 16), 1)
            + lax.broadcasted_iota(jnp.int32, (count, 16, 16), 2)
        ).astype(jnp.float32) + 0.5

        def over_bins(values):
            return jnp.sum(jnp.sum(values, axis=1, keepdims=True), axis=2, keepdims=True)

        def share_and_mean(values):
            total = over_bins(values)
            total = jnp.where(total > 0.0, total, 1.0)
            return values / total, over_bins(values * centre) / total

        own_share, own_mean = share_and_mean(own)
        other_share, other_mean = share_and_mean(other)
        gap = (own_share - other_share).reshape(count * 16, 16)
        low_a = lax.broadcasted_iota(jnp.int32, (16, 16), 0)
        low_b = lax.broadcasted_iota(jnp.int32, (16, 16), 1)
        high_a = lax.broadcasted_iota(jnp.int32, (count * 16, count * 16), 0)
        high_b = lax.broadcasted_iota(jnp.int32, (count * 16, count * 16), 1)
        within = (low_a <= low_b).astype(jnp.float32)
        before = ((high_a // 16 == high_b // 16) & (high_b < high_a)).astype(jnp.float32)
        exact = dict(precision=lax.Precision.HIGHEST, preferred_element_type=jnp.float32)
        running = jnp.dot(gap, within, **exact) + jnp.sum(
            jnp.dot(before, gap, **exact), axis=1, keepdims=True
        )
        distance = over_bins(jnp.abs(running).reshape(count, 16, 16))
        mismatch = (distance - jnp.abs(own_mean - other_mean)) / mismatch_scale
        confidence = (1.0 / (0.25 + mismatch * mismatch)).reshape(count, 1)
        offset = (jnp.log(other_mean) - jnp.log(own_mean)).reshape(count, 1)
        lane = lax.broadcasted_iota(jnp.int32, (1, lanes), 1)
        lines = [jnp.zeros((1, lanes), jnp.float32) for _ in range(rows)]
        for number, (row, column, own_side) in enumerate(pairs):
            spot = (own_side - 1) * grid_columns + x_index * columns + column
            lines[row] = jnp.where(lane == spot, confidence[number : number + 1], lines[row])
            lines[row] = jnp.where(
                lane == spot + grid_columns, offset[number : number + 1], lines[row]
            )
        return lines

    grid_rows, grid_columns = y_count * rows, x_count * columns
    number_of = {strip: n for n, strips in enumerate(groups) for strip in strips}
    def numbers_of(strips):
        return sorted({number_of[strip] for strip in strips})

    hear()
    finish(numbers_of(borders[2]))
    for row in range(rows):
        column_out[row] = hist[place_of((row, 0, 2))]

    @pl.when(present[2])
    def _():
        near_copy(1).start()

    @pl.loop(0, chunks)
    def _(index):
        await_halo(0, index)
        await_halo(1, index)
        edge(0, index)
        edge(1, index)

    finish(numbers_of(borders[0]))
    for column in range(columns):
        row_out[column] = hist[place_of((0, column, 0))]

    @pl.when(present[0])
    def _():
        near_copy(0).start()

    rest = numbers_of(borders[1] + borders[3])
    finish(rest + [n for n in range(len(inner))])

    @pl.when(present[3])
    def _():
        near_copy(1).wait_recv()

    @pl.when(jnp.logical_not(present[3]))
    def _():
        column_in[...] = jnp.zeros_like(column_in)

    early = [(r, c, 1) for r in range(rows - 1) for c in range(columns)]
    early += [(r, c, 3) for r in range(rows) for c in range(columns)]
    lines = terms(early)

    @pl.when(present[1])
    def _():
        near_copy(0).wait_recv()

    @pl.when(jnp.logical_not(present[1]))
    def _():
        row_in[...] = jnp.zeros_like(row_in)

    more = terms(borders[1])
    for row in range(rows):
        tile[row : row + 1] = lines[row] + more[row]
    board[me] = tile[...]

    def spread(index, source):
        return pltpu.make_async_remote_copy(
            src_ref=tile, dst_ref=board.at[source],
            send_sem=far_send, recv_sem=far_recv,
            device_id=device(index), device_id_type=pl.DeviceIdType.MESH,
        )

    @pl.loop(1, devices)
    def _(step):
        spread((me + step) % devices, me).start()

    for number in range(2):
        @pl.when(present[2 * number])
        def _():
            near_copy(number).wait_send()

    for direction in range(4):
        @pl.when(present[direction])
        def _():
            pltpu.make_async_remote_copy(
                src_ref=outs[direction], dst_ref=ins[direction ^ 1],
                send_sem=send_sem.at[direction], recv_sem=recv_sem.at[direction, 0],
                device_id=target[direction], device_id_type=pl.DeviceIdType.MESH,
            ).wait_send()

    if relays:
        for far in range(2):
            @pl.when(parity == far)
            def _():
                @pl.loop(0, relay_count)
                def _(index):
                    forward(far, index).wait_send()

    others = pltpu.make_async_remote_copy(
        src_ref=board.at[pl.ds(1, devices - 1)], dst_ref=board.at[pl.ds(1, devices - 1)],
        send_sem=far_send, recv_sem=far_recv,
        device_id=device((me + 1) % devices), device_id_type=pl.DeviceIdType.MESH,
    )
    others.wait_send()
    others.wait_recv()

    for place in range(y_count):
        rows_here = board[place]
        for other_x in range(1, x_count):
            rows_here += board[other_x * y_count + place]
        grid[place * rows : (place + 1) * rows] = rows_here

    adjacency_copy.wait()
    whole = grid[...]
    row_id = lax.broadcasted_iota(jnp.int32, (grid_rows, lanes), 0)
    lane_id = lax.broadcasted_iota(jnp.int32, (grid_rows, lanes), 1)

    def quantity(number, link, keep):
        values = whole if number == 0 else pltpu.roll(whole, lanes - number * grid_columns, 1)
        return jnp.where(keep, values, 0.0)

    def widened(index):
        flat = adjacency_ref[index]
        if lanes > grid_columns:
            blank = jnp.zeros((grid_rows, lanes - grid_columns), jnp.int32)
            flat = jnp.concatenate([flat, blank], axis=1)
        return flat

    keep_down = (widened(1) > 0) & (row_id < grid_rows - 1) & (lane_id < grid_columns)
    keep_right = (widened(0) > 0) & (lane_id < grid_columns - 1)
    down_conf = quantity(0, 1, keep_down)
    down_off = quantity(1, 1, keep_down)
    right_conf = quantity(2, 0, keep_right)
    right_off = quantity(3, 0, keep_right)
    up_conf, up_off = pltpu.roll(down_conf, 1, 0), -pltpu.roll(down_off, 1, 0)
    left_conf, left_off = pltpu.roll(right_conf, 1, 1), -pltpu.roll(right_off, 1, 1)
    confidence_sum = up_conf + down_conf + left_conf + right_conf
    denominator = anchor_weight + confidence_sum
    push = (
        up_conf * up_off + down_conf * down_off + left_conf * left_off + right_conf * right_off
    ) / denominator
    up_part, down_part = up_conf / denominator, down_conf / denominator
    left_part, right_part = left_conf / denominator, right_conf / denominator
    pull = confidence_sum / denominator
    tiles = grid_rows * grid_columns

    def mean_of(values):
        return jnp.sum(jnp.sum(values, axis=0, keepdims=True), axis=1, keepdims=True) / tiles

    column_sums = (
        pltpu.roll(up_part, grid_rows - 1, 0) + pltpu.roll(down_part, 1, 0)
        + pltpu.roll(left_part, lanes - 1, 1) + pltpu.roll(right_part, 1, 1)
    )
    push_mean, pull_mean = mean_of(push), mean_of(pull)
    fresh, mean = push, push_mean
    for _ in range(ITERS - 1):
        ahead = mean_of(column_sums * fresh)
        fresh = (
            up_part * pltpu.roll(fresh, 1, 0)
            + down_part * pltpu.roll(fresh, grid_rows - 1, 0)
            + left_part * pltpu.roll(fresh, 1, 1)
            + right_part * pltpu.roll(fresh, lanes - 1, 1)
            + push
        ) - pull * mean
        mean = ahead + push_mean - pull_mean * mean
    log_gain = fresh - mean_of(fresh)
    result = jnp.zeros((rows, columns), jnp.float32)
    out_row = lax.broadcasted_iota(jnp.int32, (rows, columns), 0)
    out_column = lax.broadcasted_iota(jnp.int32, (rows, columns), 1)
    for row in range(rows):
        line = jnp.sum(jnp.where(row_id == y_index * rows + row, log_gain, 0.0), axis=0, keepdims=True)
        for column in range(columns):
            value = jnp.sum(
                jnp.where(lane_id[:1] == x_index * columns + column, line, 0.0), axis=1, keepdims=True
            )
            result += jnp.where((out_row == row) & (out_column == column), value, 0.0)
    out_ref[...] = result


def body(pixels, weights, adjacency):
    rows, columns, sides, length = pixels.shape
    steps = length // 128
    chunks = chunk_count(steps)
    x_count, y_count = lax.axis_size("gx"), lax.axis_size("gy")
    devices = x_count * y_count
    lanes = -(-4 * x_count * columns // 128) * 128

    def stacked(array):
        array = array.reshape(rows, columns, sides, steps, 128)
        return array.transpose(0, 1, 3, 2, 4).reshape(rows, columns, steps * sides, 128)

    def halo(count):
        return pltpu.VMEM((steps * count, 128), jnp.bfloat16)

    halos = [halo(columns), halo(columns), halo(rows), halo(rows)]
    return pl.pallas_call(
        functools.partial(kernel, (rows, columns, steps), chunks),
        in_specs=[pl.BlockSpec(memory_space=pl.ANY)] * 3,
        out_specs=pl.BlockSpec(memory_space=pltpu.VMEM),
        out_shape=pltpu.VMEM((rows, columns), jnp.float32),
        scratch_shapes=[
            pltpu.VMEM((rows, columns, steps * sides, 128), jnp.int32),
            pltpu.VMEM((rows, columns, steps * sides, 128), jnp.bfloat16),
            *halos,
            *halos,
            pltpu.VMEM((len(all_groups(rows, columns)), 256, 256), jnp.float32),
            pltpu.VMEM((rows * columns * sides, 16, 16), jnp.float32),
            *([pltpu.VMEM((columns, 16, 16), jnp.float32), pltpu.VMEM((rows, 16, 16), jnp.float32)] * 2),
            pltpu.VMEM((rows, lanes), jnp.float32),
            pltpu.VMEM((devices, rows, lanes), jnp.float32),
            pltpu.VMEM((y_count * rows, lanes), jnp.float32),
            pltpu.VMEM(adjacency.shape, jnp.int32),
            pltpu.SemaphoreType.DMA((chunks,)),
            pltpu.SemaphoreType.DMA((chunks,)),
            pltpu.SemaphoreType.DMA((4,)),
            pltpu.SemaphoreType.DMA((4, chunks)),
            pltpu.SemaphoreType.DMA((2,)),
            pltpu.SemaphoreType.DMA((2,)),
            pltpu.SemaphoreType.DMA,
            pltpu.SemaphoreType.DMA,
            pltpu.SemaphoreType.DMA,
            halo(columns),
            pltpu.SemaphoreType.DMA((chunks,)),
            pltpu.SemaphoreType.DMA((chunks,)),
            pltpu.SemaphoreType.REGULAR((4,)),
        ],
        compiler_params=pltpu.CompilerParams(
            collective_id=0, has_side_effects=True, vmem_limit_bytes=60 * 1024 * 1024
        ),
        name="equalise",
    )(stacked(pixels), stacked(weights), adjacency)


def solution(mesh):
    return jax.shard_map(
        body,
        mesh=mesh,
        in_specs=(P("gy", "gx", None, None), P("gy", "gx", None, None), P()),
        out_specs=P("gy", "gx"),
        check_vma=False,
    )
```

```python
import functools
import jax
import jax.numpy as jnp
from jax import lax
from jax.experimental import pallas as pl
from jax.experimental.pallas import tpu as pltpu
from jax.sharding import PartitionSpec as P

ITERS = 20
CHUNKS = 8
LEVELS = 16

anchor_weight = 0.5
mismatch_scale = 8.0


def partner_of(strip):
    row, column, side = strip
    return [
        (row - 1, column, 1),
        (row + 1, column, 0),
        (row, column - 1, 3),
        (row, column + 1, 2),
    ][side]


def border(direction, rows, columns):
    return [
        [(0, column, 0) for column in range(columns)],
        [(rows - 1, column, 1) for column in range(columns)],
        [(row, 0, 2) for row in range(rows)],
        [(row, columns - 1, 3) for row in range(rows)],
    ][direction]


def groups_of(strips):
    groups, first = [], 0
    while first < len(strips):
        size = min(4, len(strips) - first)
        size = 2 if size == 3 else size
        groups.append(strips[first : first + size])
        first += size
    return groups


def inner_groups(rows, columns):
    down = [(row, column, 1) for row in range(rows - 1) for column in range(columns)]
    right = [(row, column, 3) for row in range(rows) for column in range(columns - 1)]
    groups = []
    for strips in groups_of(down) + groups_of(right):
        groups += [strips, [partner_of(strip) for strip in strips]]
    return groups


def all_groups(rows, columns):
    groups = inner_groups(rows, columns)
    for direction in range(4):
        groups += groups_of(border(direction, rows, columns))
    return groups


def roll_rows(values, shift):
    shift = shift % 8
    return values if shift == 0 else pltpu.roll(values, shift, 1)


def gather(read, strips, start, height, side):
    length = height * len(strips) // 4
    total = None
    for place in range(4):
        row, column, own = strips[place % len(strips)]
        value = read[row, column, pl.ds(start + place // len(strips) * length, length), :]
        if value.dtype == jnp.bfloat16:
            value = value.astype(jnp.float32)
        value = roll_rows(value.reshape(length // 8, 8, 128), place - own)
        total = value if total is None else jnp.where(side == place, value, total)
    return total


def flat(values, dtype):
    return values.reshape(values.shape[0] * 8, 128).astype(dtype)


def across(values):
    return jnp.concatenate([values[i : i + 16] for i in range(0, values.shape[0], 16)], axis=1)


def outer_product(bins, joint):
    bins, joint = across(bins), across(joint)
    upper, lower = bins & 240, bins & 15
    zero, one = jnp.zeros_like(joint), jnp.ones_like(joint)
    left = jnp.concatenate([jnp.where(upper == 16 * i, joint, zero) for i in range(LEVELS)], axis=0)
    right = jnp.concatenate([jnp.where(lower == i, one, zero) for i in range(LEVELS)], axis=0)
    return lax.dot_general(left, right, (((1,), (1,)), ((), ())), preferred_element_type=jnp.float32)


def chunk_count(steps):
    count = CHUNKS
    while steps % (count * 16):
        count //= 2
    return count


def kernel(
    shape, chunks, p_ref, w_ref, adjacency_hbm, out_ref,
    p_all, w_all, up_out, down_out, left_out, right_out, up_in, down_in, left_in, right_in, sums,
    hist, row_out, column_out, row_in, column_in, tile, board, grid, adjacency_ref,
    p_sem, w_sem, send_sem, recv_sem, near_send, near_recv, far_send, far_recv, adjacency_sem,
    relay_in, relay_send, relay_recv, told,
):
    rows, columns, steps = shape
    span = steps // chunks
    height = span * 4
    outs = [up_out, down_out, left_out, right_out]
    ins = [up_in, down_in, left_in, right_in]
    x_count, y_count = lax.axis_size("gx"), lax.axis_size("gy")
    x_index, y_index = lax.axis_index("gx"), lax.axis_index("gy")
    devices = x_count * y_count
    me = x_index * y_count + y_index
    present = [y_index > 0, y_index < y_count - 1, x_index > 0, x_index < x_count - 1]
    target = [
        {"gx": x_index, "gy": y_index - 1},
        {"gx": x_index, "gy": y_index + 1},
        {"gx": x_index - 1, "gy": y_index},
        {"gx": x_index + 1, "gy": y_index},
    ]
    borders = [border(d, rows, columns) for d in range(4)]
    inner = inner_groups(rows, columns)
    groups = all_groups(rows, columns)
    side = lax.broadcasted_iota(jnp.int32, (1, 8, 128), 1) % 4

    def chunk(index, size):
        return pl.ds(pl.multiple_of(index * size, 16), size)

    def fetch(index, source, target_ref, sem):
        window = chunk(index, height)
        return pltpu.make_async_copy(
            source.at[:, :, window, :], target_ref.at[:, :, window, :], sem.at[index]
        )

    def send(direction, index):
        window = chunk(index, span * len(borders[direction]))
        opposite = direction ^ 1
        return pltpu.make_async_remote_copy(
            src_ref=outs[direction].at[window, :],
            dst_ref=ins[opposite].at[window, :],
            send_sem=send_sem.at[direction],
            recv_sem=recv_sem.at[opposite, index],
            device_id=target[direction],
            device_id_type=pl.DeviceIdType.MESH,
        )

    def await_halo(direction, index):
        @pl.when(present[direction])
        def _():
            send(direction ^ 1, index).wait_recv()

    @pl.loop(0, chunks)
    def _(index):
        fetch(index, w_ref, w_all, w_sem).start()

    barrier = pltpu.get_barrier_semaphore()

    def device(index):
        return {"gx": index // y_count, "gy": index % y_count}

    greeted = list(zip(present, target))
    greeted.append((y_index > 1, {"gx": x_index, "gy": y_index - 2}))
    greeted.append((y_index < y_count - 2, {"gx": x_index, "gy": y_index + 2}))
    for here, there in greeted:
        @pl.when(here)
        def _():
            pl.semaphore_signal(barrier, inc=1, device_id=there, device_id_type=pl.DeviceIdType.MESH)

    rounds = -(-(x_count + y_count - 4) // chunks)

    def tell():
        for direction in range(4):
            @pl.when(present[direction])
            def _():
                pl.semaphore_signal(
                    told.at[direction ^ 1], inc=1, device_id=target[direction],
                    device_id_type=pl.DeviceIdType.MESH,
                )

    def hear():
        for direction in range(4):
            @pl.when(present[direction])
            def _():
                pl.semaphore_wait(told.at[direction], 1)

    def pass_word():
        for _ in range(rounds):
            hear()
            tell()

    def pack(index):
        fetch(index, w_ref, w_all, w_sem).wait()
        for direction in range(4):
            base = index * span * len(borders[direction])
            for strips in groups_of(borders[direction]):
                length = height * len(strips) // 4
                total = gather(w_all, strips, pl.multiple_of(index * height, 16), height, side)
                outs[direction][pl.ds(pl.multiple_of(base, 16), length), :] = flat(total, jnp.bfloat16)
                base += length

    relays = x_count == 4 and y_count % 2 == 0
    layers = y_count // 2
    layer, parity = y_index // 2, y_index % 2
    up_count, down_count = chunks * layer // layers, chunks * (layers - 1 - layer) // layers
    out_count = jnp.where(parity == 1, down_count, up_count)
    relay_count = jnp.where(parity == 1, up_count, down_count)
    relay_chunk = span * columns

    def to_relay(far, index):
        return pltpu.make_async_remote_copy(
            src_ref=outs[far].at[chunk(index, relay_chunk), :],
            dst_ref=relay_in.at[chunk(index, relay_chunk), :],
            send_sem=send_sem.at[far],
            recv_sem=relay_recv.at[index],
            device_id=target[1 - far],
            device_id_type=pl.DeviceIdType.MESH,
        )

    def forward(far, index):
        step = -2 if far == 1 else 2
        return pltpu.make_async_remote_copy(
            src_ref=relay_in.at[chunk(index, relay_chunk), :],
            dst_ref=ins[far].at[chunk(index, relay_chunk), :],
            send_sem=relay_send.at[index],
            recv_sem=recv_sem.at[far, index],
            device_id={"gx": x_index, "gy": y_index + step},
            device_id_type=pl.DeviceIdType.MESH,
        )

    def pass_on(index):
        piece = index - (chunks - relay_count) + 1
        for far in range(2):
            @pl.when((parity == far) & (piece >= 0) & (piece < relay_count))
            def _():
                to_relay(far, piece).wait_recv()
                forward(far, piece).start()

    def send_first(index):
        for direction in range(2, 4):
            @pl.when(present[direction])
            def _():
                send(direction, index).start()

        if not relays:
            for direction in range(2):
                @pl.when(present[direction])
                def _():
                    send(direction, index).start()
            return

        for far in range(2):
            @pl.when((parity == far) & present[far] & (index < out_count))
            def _():
                to_relay(far, index).start()

            @pl.when((parity == far) & present[far] & (index >= out_count))
            def _():
                send(far, index).start()

            @pl.when((parity == far) & (out_count == 0))
            def _():
                send(1 - far, index).start()

    def send_rest():
        if not relays:
            return
        for far in range(2):
            @pl.when((parity == far) & (out_count > 0))
            def _():
                @pl.loop(0, chunks)
                def _(index):
                    send(1 - far, index).start()

    @pl.loop(0, chunks)
    def _(index):
        fetch(index, p_ref, p_all, p_sem).start()

    adjacency_copy = pltpu.make_async_copy(adjacency_hbm, adjacency_ref, adjacency_sem)
    adjacency_copy.start()
    pack(0)
    pl.semaphore_wait(barrier, sum(jnp.where(here, 1, 0) for here, _ in greeted))
    tell()

    @pl.loop(1, chunks)
    def _(index):
        pack(index)
        send_first(index - 1)

    send_first(chunks - 1)
    send_rest()

    for direction in range(4):
        @pl.when(jnp.logical_not(present[direction]))
        def _():
            ins[direction][...] = jnp.zeros_like(ins[direction])

    def clear(first, count):
        sums[first : first + count] = jnp.zeros((count, 256, 256), jnp.float32)

    clear(0, len(groups))
    for number in sorted({groups.index(g) for d in range(2) for g in groups_of(borders[d])}):
        clear(number + len(groups), 1)

    def bins_of(strips, index):
        return flat(gather(p_all, strips, pl.multiple_of(index * height, 16), height, side), jnp.int16)

    def edge(direction, index, spare=0):
        base = index * span * len(borders[direction])
        for strips in groups_of(borders[direction]):
            length = height * len(strips) // 4
            window = pl.ds(pl.multiple_of(base, 16), length)
            mine = outs[direction][window, :].astype(jnp.float32)
            joint = (mine * ins[direction][window, :].astype(jnp.float32)).astype(jnp.bfloat16)
            sums[groups.index(strips) + spare * len(groups)] += outer_product(bins_of(strips, index), joint)
            base += length

    @pl.loop(0, chunks)
    def _(index):
        pass_word()
        if relays:
            pass_on(index)
        fetch(index, p_ref, p_all, p_sem).wait()
        await_halo(2, index)
        await_halo(3, index)
        for number in range(0, len(inner), 2):
            start = pl.multiple_of(index * height, 16)
            first = gather(w_all, inner[number], start, height, side)
            second = gather(w_all, inner[number + 1], start, height, side)
            joint = flat(first * second, jnp.bfloat16)
            sums[number] += outer_product(bins_of(inner[number], index), joint)
            sums[number + 1] += outer_product(bins_of(inner[number + 1], index), joint)
        edge(2, index)
        edge(3, index)

    near = [
        (row_out, row_in, near_send.at[0], near_recv.at[0], target[0]),
        (column_out, column_in, near_send.at[1], near_recv.at[1], target[2]),
    ]

    def near_copy(number):
        source, destination, send_side, recv_side, where = near[number]
        return pltpu.make_async_remote_copy(
            src_ref=source, dst_ref=destination, send_sem=send_side, recv_sem=recv_side,
            device_id=where, device_id_type=pl.DeviceIdType.MESH,
        )

    grid_rows, grid_columns = y_count * rows, x_count * columns
    number_of = {strip: n for n, strips in enumerate(groups) for strip in strips}
    def numbers_of(strips):
        return sorted({number_of[strip] for strip in strips})

    pair = 2 if chunks % 2 == 0 else 1

    def finish(numbers):
        a = lax.broadcasted_iota(jnp.int32, (256, 256), 0)
        b = lax.broadcasted_iota(jnp.int32, (256, 256), 1)
        halves = numbers_of(borders[0] + borders[1]) if pair == 2 else []
        packed = []
        for number in numbers:
            total = sums[number]
            if number in halves:
                total += sums[number + len(groups)]
            kept = jnp.where(a % 16 == b % 16, total, 0.0)
            packed.append(jnp.sum(kept.reshape(16, 16, 256), axis=1))
        packed = jnp.concatenate(packed, axis=0)
        lane = lax.broadcasted_iota(jnp.int32, (256, 64), 0)
        spot = lax.broadcasted_iota(jnp.int32, (256, 64), 1)
        pick = ((lane // 16 == spot % 16) & (lane % 4 == spot // 16)).astype(jnp.float32)
        result = jnp.dot(packed, pick, precision=lax.Precision.HIGHEST, preferred_element_type=jnp.float32)
        for order, number in enumerate(numbers):
            strips = groups[number]
            for first, strip in enumerate(strips):
                parts = [
                    result[order * 16 : order * 16 + 16, place * 16 : place * 16 + 16]
                    for place in range(first, 4, len(strips))
                ]
                hist[place_of(strip)] = sum(parts[1:], parts[0])

    def place_of(strip):
        row, column, own = strip
        return (row * columns + column) * 4 + own

    lanes = grid.shape[1]

    def terms(pairs):
        count = len(pairs)
        own = jnp.stack([hist[place_of(strip)] for strip in pairs])
        other = []
        for strip in pairs:
            row, column, _ = partner_of(strip)
            if row == rows:
                other.append(row_in[column])
            elif column == columns:
                other.append(column_in[row])
            else:
                other.append(hist[place_of(partner_of(strip))])
        other = jnp.stack(other)
        centre = (
            16 * lax.broadcasted_iota(jnp.int32, (count, 16, 16), 1)
            + lax.broadcasted_iota(jnp.int32, (count, 16, 16), 2)
        ).astype(jnp.float32) + 0.5

        def over_bins(values):
            return jnp.sum(jnp.sum(values, axis=1, keepdims=True), axis=2, keepdims=True)

        def share_and_mean(values):
            total = over_bins(values)
            total = jnp.where(total > 0.0, total, 1.0)
            return values / total, over_bins(values * centre) / total

        own_share, own_mean = share_and_mean(own)
        other_share, other_mean = share_and_mean(other)
        gap = (own_share - other_share).reshape(count * 16, 16)
        low_a = lax.broadcasted_iota(jnp.int32, (16, 16), 0)
        low_b = lax.broadcasted_iota(jnp.int32, (16, 16), 1)
        high_a = lax.broadcasted_iota(jnp.int32, (count * 16, count * 16), 0)
        high_b = lax.broadcasted_iota(jnp.int32, (count * 16, count * 16), 1)
        within = (low_a <= low_b).astype(jnp.float32)
        before = ((high_a // 16 == high_b // 16) & (high_b < high_a)).astype(jnp.float32)
        exact = dict(precision=lax.Precision.HIGHEST, preferred_element_type=jnp.float32)
        running = jnp.dot(gap, within, **exact) + jnp.sum(
            jnp.dot(before, gap, **exact), axis=1, keepdims=True
        )
        distance = over_bins(jnp.abs(running).reshape(count, 16, 16))
        mismatch = (distance - jnp.abs(own_mean - other_mean)) / mismatch_scale
        confidence = (1.0 / (0.25 + mismatch * mismatch)).reshape(count, 1)
        offset = (jnp.log(other_mean) - jnp.log(own_mean)).reshape(count, 1)
        lane = lax.broadcasted_iota(jnp.int32, (1, lanes), 1)
        lines = [jnp.zeros((1, lanes), jnp.float32) for _ in range(rows)]
        for number, (row, column, own_side) in enumerate(pairs):
            spot = (own_side - 1) * grid_columns + x_index * columns + column
            lines[row] = jnp.where(lane == spot, confidence[number : number + 1], lines[row])
            lines[row] = jnp.where(
                lane == spot + grid_columns, offset[number : number + 1], lines[row]
            )
        return lines

    hear()
    finish(numbers_of(borders[2]))
    for row in range(rows):
        column_out[row] = hist[place_of((row, 0, 2))]

    @pl.when(present[2])
    def _():
        near_copy(1).start()

    def border_pass(direction):
        @pl.loop(0, chunks // pair)
        def _(index):
            for spare in range(pair):
                await_halo(direction, index * pair + spare)
            for spare in range(pair):
                edge(direction, index * pair + spare, spare)

    def send_up_sums():
        finish(numbers_of(borders[0]))
        for column in range(columns):
            row_out[column] = hist[place_of((0, column, 0))]

        @pl.when(present[0])
        def _():
            near_copy(0).start()

    @pl.when(parity == 0)
    def _():
        border_pass(0)
        send_up_sums()
        border_pass(1)

    @pl.when(parity == 1)
    def _():
        border_pass(1)
        border_pass(0)
        send_up_sums()

    rest = numbers_of(borders[1] + borders[3])
    finish(rest + [n for n in range(len(inner))])

    @pl.when(present[3])
    def _():
        near_copy(1).wait_recv()

    @pl.when(jnp.logical_not(present[3]))
    def _():
        column_in[...] = jnp.zeros_like(column_in)

    early = [(r, c, 1) for r in range(rows - 1) for c in range(columns)]
    early += [(r, c, 3) for r in range(rows) for c in range(columns)]
    lines = terms(early)

    @pl.when(present[1])
    def _():
        near_copy(0).wait_recv()

    @pl.when(jnp.logical_not(present[1]))
    def _():
        row_in[...] = jnp.zeros_like(row_in)

    more = terms(borders[1])
    for row in range(rows):
        tile[row : row + 1] = lines[row] + more[row]
    board[me] = tile[...]

    def spread(index, source):
        return pltpu.make_async_remote_copy(
            src_ref=tile, dst_ref=board.at[source],
            send_sem=far_send, recv_sem=far_recv,
            device_id=device(index), device_id_type=pl.DeviceIdType.MESH,
        )

    @pl.loop(1, devices)
    def _(step):
        spread((me + step) % devices, me).start()

    for number in range(2):
        @pl.when(present[2 * number])
        def _():
            near_copy(number).wait_send()

    for direction in range(4):
        @pl.when(present[direction])
        def _():
            pltpu.make_async_remote_copy(
                src_ref=outs[direction], dst_ref=ins[direction ^ 1],
                send_sem=send_sem.at[direction], recv_sem=recv_sem.at[direction, 0],
                device_id=target[direction], device_id_type=pl.DeviceIdType.MESH,
            ).wait_send()

    if relays:
        for far in range(2):
            @pl.when(parity == far)
            def _():
                @pl.loop(0, relay_count)
                def _(index):
                    forward(far, index).wait_send()

    others = pltpu.make_async_remote_copy(
        src_ref=board.at[pl.ds(1, devices - 1)], dst_ref=board.at[pl.ds(1, devices - 1)],
        send_sem=far_send, recv_sem=far_recv,
        device_id=device((me + 1) % devices), device_id_type=pl.DeviceIdType.MESH,
    )
    others.wait_send()
    others.wait_recv()

    for place in range(y_count):
        rows_here = board[place]
        for other_x in range(1, x_count):
            rows_here += board[other_x * y_count + place]
        grid[place * rows : (place + 1) * rows] = rows_here

    adjacency_copy.wait()
    whole = grid[...]
    row_id = lax.broadcasted_iota(jnp.int32, (grid_rows, lanes), 0)
    lane_id = lax.broadcasted_iota(jnp.int32, (grid_rows, lanes), 1)

    def quantity(number, link, keep):
        values = whole if number == 0 else pltpu.roll(whole, lanes - number * grid_columns, 1)
        return jnp.where(keep, values, 0.0)

    def widened(index):
        flat = adjacency_ref[index]
        if lanes > grid_columns:
            blank = jnp.zeros((grid_rows, lanes - grid_columns), jnp.int32)
            flat = jnp.concatenate([flat, blank], axis=1)
        return flat

    keep_down = (widened(1) > 0) & (row_id < grid_rows - 1) & (lane_id < grid_columns)
    keep_right = (widened(0) > 0) & (lane_id < grid_columns - 1)
    down_conf = quantity(0, 1, keep_down)
    down_off = quantity(1, 1, keep_down)
    right_conf = quantity(2, 0, keep_right)
    right_off = quantity(3, 0, keep_right)
    up_conf, up_off = pltpu.roll(down_conf, 1, 0), -pltpu.roll(down_off, 1, 0)
    left_conf, left_off = pltpu.roll(right_conf, 1, 1), -pltpu.roll(right_off, 1, 1)
    confidence_sum = up_conf + down_conf + left_conf + right_conf
    denominator = anchor_weight + confidence_sum
    push = (
        up_conf * up_off + down_conf * down_off + left_conf * left_off + right_conf * right_off
    ) / denominator
    up_part, down_part = up_conf / denominator, down_conf / denominator
    left_part, right_part = left_conf / denominator, right_conf / denominator
    pull = confidence_sum / denominator
    tiles = grid_rows * grid_columns

    def mean_of(values):
        return jnp.sum(jnp.sum(values, axis=0, keepdims=True), axis=1, keepdims=True) / tiles

    column_sums = (
        pltpu.roll(up_part, grid_rows - 1, 0) + pltpu.roll(down_part, 1, 0)
        + pltpu.roll(left_part, lanes - 1, 1) + pltpu.roll(right_part, 1, 1)
    )
    push_mean, pull_mean = mean_of(push), mean_of(pull)
    fresh, mean = push, push_mean
    for _ in range(ITERS - 1):
        ahead = mean_of(column_sums * fresh)
        fresh = (
            up_part * pltpu.roll(fresh, 1, 0)
            + down_part * pltpu.roll(fresh, grid_rows - 1, 0)
            + left_part * pltpu.roll(fresh, 1, 1)
            + right_part * pltpu.roll(fresh, lanes - 1, 1)
            + push
        ) - pull * mean
        mean = ahead + push_mean - pull_mean * mean
    log_gain = fresh - mean_of(fresh)
    result = jnp.zeros((rows, columns), jnp.float32)
    out_row = lax.broadcasted_iota(jnp.int32, (rows, columns), 0)
    out_column = lax.broadcasted_iota(jnp.int32, (rows, columns), 1)
    for row in range(rows):
        line = jnp.sum(jnp.where(row_id == y_index * rows + row, log_gain, 0.0), axis=0, keepdims=True)
        for column in range(columns):
            value = jnp.sum(
                jnp.where(lane_id[:1] == x_index * columns + column, line, 0.0), axis=1, keepdims=True
            )
            result += jnp.where((out_row == row) & (out_column == column), value, 0.0)
    out_ref[...] = result


def body(pixels, weights, adjacency):
    rows, columns, sides, length = pixels.shape
    steps = length // 128
    chunks = chunk_count(steps)
    x_count, y_count = lax.axis_size("gx"), lax.axis_size("gy")
    devices = x_count * y_count
    lanes = -(-4 * x_count * columns // 128) * 128

    def stacked(array):
        array = array.reshape(rows, columns, sides, steps, 128)
        return array.transpose(0, 1, 3, 2, 4).reshape(rows, columns, steps * sides, 128)

    def halo(count):
        return pltpu.VMEM((steps * count, 128), jnp.bfloat16)

    halos = [halo(columns), halo(columns), halo(rows), halo(rows)]
    return pl.pallas_call(
        functools.partial(kernel, (rows, columns, steps), chunks),
        in_specs=[pl.BlockSpec(memory_space=pl.ANY)] * 3,
        out_specs=pl.BlockSpec(memory_space=pltpu.VMEM),
        out_shape=pltpu.VMEM((rows, columns), jnp.float32),
        scratch_shapes=[
            pltpu.VMEM((rows, columns, steps * sides, 128), jnp.int32),
            pltpu.VMEM((rows, columns, steps * sides, 128), jnp.bfloat16),
            *halos,
            *halos,
            pltpu.VMEM((2 * len(all_groups(rows, columns)), 256, 256), jnp.float32),
            pltpu.VMEM((rows * columns * sides, 16, 16), jnp.float32),
            *([pltpu.VMEM((columns, 16, 16), jnp.float32), pltpu.VMEM((rows, 16, 16), jnp.float32)] * 2),
            pltpu.VMEM((rows, lanes), jnp.float32),
            pltpu.VMEM((devices, rows, lanes), jnp.float32),
            pltpu.VMEM((y_count * rows, lanes), jnp.float32),
            pltpu.VMEM(adjacency.shape, jnp.int32),
            pltpu.SemaphoreType.DMA((chunks,)),
            pltpu.SemaphoreType.DMA((chunks,)),
            pltpu.SemaphoreType.DMA((4,)),
            pltpu.SemaphoreType.DMA((4, chunks)),
            pltpu.SemaphoreType.DMA((2,)),
            pltpu.SemaphoreType.DMA((2,)),
            pltpu.SemaphoreType.DMA,
            pltpu.SemaphoreType.DMA,
            pltpu.SemaphoreType.DMA,
            halo(columns),
            pltpu.SemaphoreType.DMA((chunks,)),
            pltpu.SemaphoreType.DMA((chunks,)),
            pltpu.SemaphoreType.REGULAR((4,)),
        ],
        compiler_params=pltpu.CompilerParams(
            collective_id=0, has_side_effects=True, vmem_limit_bytes=60 * 1024 * 1024
        ),
        name="equalise",
    )(stacked(pixels), stacked(weights), adjacency)


def solution(mesh):
    return jax.shard_map(
        body,
        mesh=mesh,
        in_specs=(P("gy", "gx", None, None), P("gy", "gx", None, None), P()),
        out_specs=P("gy", "gx"),
        check_vma=False,
    )
```

```python
import functools
import jax
import jax.numpy as jnp
from jax import lax
from jax.experimental import pallas as pl
from jax.experimental.pallas import tpu as pltpu
from jax.sharding import PartitionSpec as P

ITERS = 20
CHUNKS = 8
LEVELS = 16

anchor_weight = 0.5
mismatch_scale = 8.0


def partner_of(strip):
    row, column, side = strip
    return [
        (row - 1, column, 1),
        (row + 1, column, 0),
        (row, column - 1, 3),
        (row, column + 1, 2),
    ][side]


def border(direction, rows, columns):
    return [
        [(0, column, 0) for column in range(columns)],
        [(rows - 1, column, 1) for column in range(columns)],
        [(row, 0, 2) for row in range(rows)],
        [(row, columns - 1, 3) for row in range(rows)],
    ][direction]


def groups_of(strips):
    groups, first = [], 0
    while first < len(strips):
        size = min(4, len(strips) - first)
        size = 2 if size == 3 else size
        groups.append(strips[first : first + size])
        first += size
    return groups


def inner_groups(rows, columns):
    down = [(row, column, 1) for row in range(rows - 1) for column in range(columns)]
    right = [(row, column, 3) for row in range(rows) for column in range(columns - 1)]
    groups = []
    for strips in groups_of(down) + groups_of(right):
        groups += [strips, [partner_of(strip) for strip in strips]]
    return groups


def all_groups(rows, columns):
    groups = inner_groups(rows, columns)
    for direction in range(4):
        groups += groups_of(border(direction, rows, columns))
    return groups


def roll_rows(values, shift):
    shift = shift % 8
    return values if shift == 0 else pltpu.roll(values, shift, 1)


def gather(read, strips, start, height, side):
    length = height * len(strips) // 4
    total = None
    for place in range(4):
        row, column, own = strips[place % len(strips)]
        value = read[row, column, pl.ds(start + place // len(strips) * length, length), :]
        if value.dtype == jnp.bfloat16:
            value = value.astype(jnp.float32)
        value = roll_rows(value.reshape(length // 8, 8, 128), place - own)
        total = value if total is None else jnp.where(side == place, value, total)
    return total


def flat(values, dtype):
    return values.reshape(values.shape[0] * 8, 128).astype(dtype)


def across(values):
    return jnp.concatenate([values[i : i + 16] for i in range(0, values.shape[0], 16)], axis=1)


def outer_product(bins, joint):
    bins, joint = across(bins), across(joint)
    upper, lower = bins & 240, bins & 15
    zero, one = jnp.zeros_like(joint), jnp.ones_like(joint)
    left = jnp.concatenate([jnp.where(upper == 16 * i, joint, zero) for i in range(LEVELS)], axis=0)
    right = jnp.concatenate([jnp.where(lower == i, one, zero) for i in range(LEVELS)], axis=0)
    return lax.dot_general(left, right, (((1,), (1,)), ((), ())), preferred_element_type=jnp.float32)


def chunk_count(steps):
    count = CHUNKS
    while steps % (count * 16):
        count //= 2
    return count


def kernel(
    shape, chunks, p_ref, w_ref, adjacency_hbm, out_ref,
    p_all, w_all, up_out, down_out, left_out, right_out, up_in, down_in, left_in, right_in, sums,
    hist, row_out, column_out, row_in, column_in, tile, board, grid, adjacency_ref,
    p_sem, w_sem, send_sem, recv_sem, near_send, near_recv, far_send, far_recv, adjacency_sem,
    relay_in, relay_send, relay_recv, told,
):
    rows, columns, steps = shape
    span = steps // chunks
    height = span * 4
    outs = [up_out, down_out, left_out, right_out]
    ins = [up_in, down_in, left_in, right_in]
    x_count, y_count = lax.axis_size("gx"), lax.axis_size("gy")
    x_index, y_index = lax.axis_index("gx"), lax.axis_index("gy")
    devices = x_count * y_count
    me = x_index * y_count + y_index
    present = [y_index > 0, y_index < y_count - 1, x_index > 0, x_index < x_count - 1]
    target = [
        {"gx": x_index, "gy": y_index - 1},
        {"gx": x_index, "gy": y_index + 1},
        {"gx": x_index - 1, "gy": y_index},
        {"gx": x_index + 1, "gy": y_index},
    ]
    borders = [border(d, rows, columns) for d in range(4)]
    inner = inner_groups(rows, columns)
    groups = all_groups(rows, columns)
    side = lax.broadcasted_iota(jnp.int32, (1, 8, 128), 1) % 4

    def chunk(index, size):
        return pl.ds(pl.multiple_of(index * size, 16), size)

    def fetch(index, source, target_ref, sem):
        window = chunk(index, height)
        return pltpu.make_async_copy(
            source.at[:, :, window, :], target_ref.at[:, :, window, :], sem.at[index]
        )

    def send(direction, index):
        window = chunk(index, span * len(borders[direction]))
        opposite = direction ^ 1
        return pltpu.make_async_remote_copy(
            src_ref=outs[direction].at[window, :],
            dst_ref=ins[opposite].at[window, :],
            send_sem=send_sem.at[direction],
            recv_sem=recv_sem.at[opposite, index],
            device_id=target[direction],
            device_id_type=pl.DeviceIdType.MESH,
        )

    def await_halo(direction, index):
        @pl.when(present[direction])
        def _():
            send(direction ^ 1, index).wait_recv()

    @pl.loop(0, chunks)
    def _(index):
        fetch(index, w_ref, w_all, w_sem).start()

    barrier = pltpu.get_barrier_semaphore()

    def device(index):
        return {"gx": index // y_count, "gy": index % y_count}

    greeted = list(zip(present, target))
    greeted.append((y_index > 1, {"gx": x_index, "gy": y_index - 2}))
    greeted.append((y_index < y_count - 2, {"gx": x_index, "gy": y_index + 2}))
    for here, there in greeted:
        @pl.when(here)
        def _():
            pl.semaphore_signal(barrier, inc=1, device_id=there, device_id_type=pl.DeviceIdType.MESH)

    rounds = -(-(x_count + y_count - 4) // chunks)

    def tell():
        for direction in range(4):
            @pl.when(present[direction])
            def _():
                pl.semaphore_signal(
                    told.at[direction ^ 1], inc=1, device_id=target[direction],
                    device_id_type=pl.DeviceIdType.MESH,
                )

    def hear():
        for direction in range(4):
            @pl.when(present[direction])
            def _():
                pl.semaphore_wait(told.at[direction], 1)

    def pass_word():
        for _ in range(rounds):
            hear()
            tell()

    def pack(index):
        fetch(index, w_ref, w_all, w_sem).wait()
        for direction in range(4):
            base = index * span * len(borders[direction])
            for strips in groups_of(borders[direction]):
                length = height * len(strips) // 4
                total = gather(w_all, strips, pl.multiple_of(index * height, 16), height, side)
                outs[direction][pl.ds(pl.multiple_of(base, 16), length), :] = flat(total, jnp.bfloat16)
                base += length

    relays = x_count == 4 and y_count % 2 == 0
    layers = y_count // 2
    layer, parity = y_index // 2, y_index % 2
    up_count, down_count = chunks * layer // layers, chunks * (layers - 1 - layer) // layers
    out_count = jnp.where(parity == 1, down_count, up_count)
    relay_count = jnp.where(parity == 1, up_count, down_count)
    relay_chunk = span * columns

    def to_relay(far, index):
        return pltpu.make_async_remote_copy(
            src_ref=outs[far].at[chunk(index, relay_chunk), :],
            dst_ref=relay_in.at[chunk(index, relay_chunk), :],
            send_sem=send_sem.at[far],
            recv_sem=relay_recv.at[index],
            device_id=target[1 - far],
            device_id_type=pl.DeviceIdType.MESH,
        )

    def forward(far, index):
        step = -2 if far == 1 else 2
        return pltpu.make_async_remote_copy(
            src_ref=relay_in.at[chunk(index, relay_chunk), :],
            dst_ref=ins[far].at[chunk(index, relay_chunk), :],
            send_sem=relay_send.at[index],
            recv_sem=recv_sem.at[far, index],
            device_id={"gx": x_index, "gy": y_index + step},
            device_id_type=pl.DeviceIdType.MESH,
        )

    def pass_on(index):
        piece = index - (chunks - relay_count) + 1
        for far in range(2):
            @pl.when((parity == far) & (piece >= 0) & (piece < relay_count))
            def _():
                to_relay(far, piece).wait_recv()
                forward(far, piece).start()

    def send_first(index):
        for direction in range(2, 4):
            @pl.when(present[direction])
            def _():
                send(direction, index).start()

        if not relays:
            for direction in range(2):
                @pl.when(present[direction])
                def _():
                    send(direction, index).start()
            return

        for far in range(2):
            @pl.when((parity == far) & present[far] & (index < out_count))
            def _():
                to_relay(far, index).start()

            @pl.when((parity == far) & present[far] & (index >= out_count))
            def _():
                send(far, index).start()

            @pl.when((parity == far) & (out_count == 0))
            def _():
                send(1 - far, index).start()

    def send_rest():
        if not relays:
            return
        for far in range(2):
            @pl.when((parity == far) & (out_count > 0))
            def _():
                @pl.loop(0, chunks)
                def _(index):
                    send(1 - far, index).start()

    @pl.loop(0, chunks)
    def _(index):
        fetch(index, p_ref, p_all, p_sem).start()

    adjacency_copy = pltpu.make_async_copy(adjacency_hbm, adjacency_ref, adjacency_sem)
    adjacency_copy.start()
    for direction in range(4):
        @pl.when(jnp.logical_not(present[direction]))
        def _():
            ins[direction][...] = jnp.zeros_like(ins[direction])

    def clear(first, count):
        sums[first : first + count] = jnp.zeros((count, 256, 256), jnp.float32)

    clear(0, len(groups))
    for number in sorted({groups.index(g) for d in range(2) for g in groups_of(borders[d])}):
        clear(number + len(groups), 1)

    pack(0)
    pl.semaphore_wait(barrier, sum(jnp.where(here, 1, 0) for here, _ in greeted))
    tell()

    @pl.loop(1, chunks)
    def _(index):
        pack(index)
        send_first(index - 1)

    send_first(chunks - 1)
    send_rest()

    def bins_of(strips, index):
        return flat(gather(p_all, strips, pl.multiple_of(index * height, 16), height, side), jnp.int16)

    def edge(direction, index, spare=0, split=1):
        base = index * span * len(borders[direction])
        for strips in groups_of(borders[direction]):
            length = height * len(strips) // 4
            window = pl.ds(pl.multiple_of(base, 16), length)
            mine = outs[direction][window, :].astype(jnp.float32)
            joint = (mine * ins[direction][window, :].astype(jnp.float32)).astype(jnp.bfloat16)
            bins, piece = bins_of(strips, index), length // split
            for number in range(split):
                part = slice(number * piece, number * piece + piece)
                place = groups.index(strips) + (spare + number) * len(groups)
                sums[place] += outer_product(bins[part], joint[part])
            base += length

    @pl.loop(0, chunks)
    def _(index):
        pass_word()
        if relays:
            pass_on(index)
        fetch(index, p_ref, p_all, p_sem).wait()
        await_halo(2, index)
        await_halo(3, index)
        for number in range(0, len(inner), 2):
            start = pl.multiple_of(index * height, 16)
            first = gather(w_all, inner[number], start, height, side)
            second = gather(w_all, inner[number + 1], start, height, side)
            joint = flat(first * second, jnp.bfloat16)
            sums[number] += outer_product(bins_of(inner[number], index), joint)
            sums[number + 1] += outer_product(bins_of(inner[number + 1], index), joint)
        edge(2, index)
        edge(3, index)

    near = [
        (row_out, row_in, near_send.at[0], near_recv.at[0], target[0]),
        (column_out, column_in, near_send.at[1], near_recv.at[1], target[2]),
    ]

    def near_copy(number):
        source, destination, send_side, recv_side, where = near[number]
        return pltpu.make_async_remote_copy(
            src_ref=source, dst_ref=destination, send_sem=send_side, recv_sem=recv_side,
            device_id=where, device_id_type=pl.DeviceIdType.MESH,
        )

    grid_rows, grid_columns = y_count * rows, x_count * columns
    number_of = {strip: n for n, strips in enumerate(groups) for strip in strips}
    def numbers_of(strips):
        return sorted({number_of[strip] for strip in strips})

    pair = 2 if chunks % 2 == 0 else 1

    def finish(numbers):
        a = lax.broadcasted_iota(jnp.int32, (256, 256), 0)
        b = lax.broadcasted_iota(jnp.int32, (256, 256), 1)
        halves = numbers_of(borders[0] + borders[1]) if pair == 2 else []
        packed = []
        for number in numbers:
            total = sums[number]
            if number in halves:
                total += sums[number + len(groups)]
            kept = jnp.where(a % 16 == b % 16, total, 0.0)
            packed.append(jnp.sum(kept.reshape(16, 16, 256), axis=1))
        packed = jnp.concatenate(packed, axis=0)
        lane = lax.broadcasted_iota(jnp.int32, (256, 64), 0)
        spot = lax.broadcasted_iota(jnp.int32, (256, 64), 1)
        pick = ((lane // 16 == spot % 16) & (lane % 4 == spot // 16)).astype(jnp.float32)
        result = jnp.dot(packed, pick, precision=lax.Precision.HIGHEST, preferred_element_type=jnp.float32)
        for order, number in enumerate(numbers):
            strips = groups[number]
            for first, strip in enumerate(strips):
                parts = [
                    result[order * 16 : order * 16 + 16, place * 16 : place * 16 + 16]
                    for place in range(first, 4, len(strips))
                ]
                hist[place_of(strip)] = sum(parts[1:], parts[0])

    def place_of(strip):
        row, column, own = strip
        return (row * columns + column) * 4 + own

    lanes = grid.shape[1]

    def terms(pairs):
        count = len(pairs)
        own = jnp.stack([hist[place_of(strip)] for strip in pairs])
        other = []
        for strip in pairs:
            row, column, _ = partner_of(strip)
            if row == rows:
                other.append(row_in[column])
            elif column == columns:
                other.append(column_in[row])
            else:
                other.append(hist[place_of(partner_of(strip))])
        other = jnp.stack(other)
        centre = (
            16 * lax.broadcasted_iota(jnp.int32, (count, 16, 16), 1)
            + lax.broadcasted_iota(jnp.int32, (count, 16, 16), 2)
        ).astype(jnp.float32) + 0.5

        def over_bins(values):
            return jnp.sum(jnp.sum(values, axis=1, keepdims=True), axis=2, keepdims=True)

        def share_and_mean(values):
            total = over_bins(values)
            total = jnp.where(total > 0.0, total, 1.0)
            return values / total, over_bins(values * centre) / total

        own_share, own_mean = share_and_mean(own)
        other_share, other_mean = share_and_mean(other)
        gap = (own_share - other_share).reshape(count * 16, 16)
        low_a = lax.broadcasted_iota(jnp.int32, (16, 16), 0)
        low_b = lax.broadcasted_iota(jnp.int32, (16, 16), 1)
        high_a = lax.broadcasted_iota(jnp.int32, (count * 16, count * 16), 0)
        high_b = lax.broadcasted_iota(jnp.int32, (count * 16, count * 16), 1)
        within = (low_a <= low_b).astype(jnp.float32)
        before = ((high_a // 16 == high_b // 16) & (high_b < high_a)).astype(jnp.float32)
        exact = dict(precision=lax.Precision.HIGHEST, preferred_element_type=jnp.float32)
        running = jnp.dot(gap, within, **exact) + jnp.sum(
            jnp.dot(before, gap, **exact), axis=1, keepdims=True
        )
        distance = over_bins(jnp.abs(running).reshape(count, 16, 16))
        mismatch = (distance - jnp.abs(own_mean - other_mean)) / mismatch_scale
        confidence = (1.0 / (0.25 + mismatch * mismatch)).reshape(count, 1)
        offset = (jnp.log(other_mean) - jnp.log(own_mean)).reshape(count, 1)
        lane = lax.broadcasted_iota(jnp.int32, (1, lanes), 1)
        lines = [jnp.zeros((1, lanes), jnp.float32) for _ in range(rows)]
        for number, (row, column, own_side) in enumerate(pairs):
            spot = (own_side - 1) * grid_columns + x_index * columns + column
            lines[row] = jnp.where(lane == spot, confidence[number : number + 1], lines[row])
            lines[row] = jnp.where(
                lane == spot + grid_columns, offset[number : number + 1], lines[row]
            )
        return lines

    hear()
    finish(numbers_of(borders[2]))
    for row in range(rows):
        column_out[row] = hist[place_of((row, 0, 2))]

    @pl.when(present[2])
    def _():
        near_copy(1).start()

    def border_pass(direction, last):
        apart = last and pair == 2 and span % 32 == 0

        @pl.loop(0, chunks // pair - apart)
        def _(index):
            for spare in range(pair):
                await_halo(direction, index * pair + spare)
            for spare in range(pair):
                edge(direction, index * pair + spare, spare)

        if apart:
            for index in range(chunks - 2, chunks):
                await_halo(direction, index)
                edge(direction, index, split=2)

    def send_up_sums():
        finish(numbers_of(borders[0]))
        for column in range(columns):
            row_out[column] = hist[place_of((0, column, 0))]

        @pl.when(present[0])
        def _():
            near_copy(0).start()

    @pl.when(parity == 0)
    def _():
        border_pass(0, False)
        send_up_sums()
        border_pass(1, True)

    @pl.when(parity == 1)
    def _():
        border_pass(1, False)
        border_pass(0, True)
        send_up_sums()

    rest = numbers_of(borders[1] + borders[3])
    finish(rest + [n for n in range(len(inner))])

    @pl.when(present[3])
    def _():
        near_copy(1).wait_recv()

    @pl.when(jnp.logical_not(present[3]))
    def _():
        column_in[...] = jnp.zeros_like(column_in)

    early = [(r, c, 1) for r in range(rows - 1) for c in range(columns)]
    early += [(r, c, 3) for r in range(rows) for c in range(columns)]
    lines = terms(early)

    @pl.when(present[1])
    def _():
        near_copy(0).wait_recv()

    @pl.when(jnp.logical_not(present[1]))
    def _():
        row_in[...] = jnp.zeros_like(row_in)

    more = terms(borders[1])
    for row in range(rows):
        tile[row : row + 1] = lines[row] + more[row]
    board[me] = tile[...]

    def spread(index, source):
        return pltpu.make_async_remote_copy(
            src_ref=tile, dst_ref=board.at[source],
            send_sem=far_send, recv_sem=far_recv,
            device_id=device(index), device_id_type=pl.DeviceIdType.MESH,
        )

    @pl.loop(0, devices)
    def _(step):
        line = step // x_count
        farthest = jnp.where(2 * y_index < y_count, y_count - 1 - line, line)
        index = (step % x_count) * y_count + farthest

        @pl.when(index != me)
        def _():
            spread(index, me).start()

    for number in range(2):
        @pl.when(present[2 * number])
        def _():
            near_copy(number).wait_send()

    for direction in range(4):
        @pl.when(present[direction])
        def _():
            pltpu.make_async_remote_copy(
                src_ref=outs[direction], dst_ref=ins[direction ^ 1],
                send_sem=send_sem.at[direction], recv_sem=recv_sem.at[direction, 0],
                device_id=target[direction], device_id_type=pl.DeviceIdType.MESH,
            ).wait_send()

    if relays:
        for far in range(2):
            @pl.when(parity == far)
            def _():
                @pl.loop(0, relay_count)
                def _(index):
                    forward(far, index).wait_send()

    others = pltpu.make_async_remote_copy(
        src_ref=board.at[pl.ds(1, devices - 1)], dst_ref=board.at[pl.ds(1, devices - 1)],
        send_sem=far_send, recv_sem=far_recv,
        device_id=device((me + 1) % devices), device_id_type=pl.DeviceIdType.MESH,
    )
    others.wait_send()
    others.wait_recv()

    for place in range(y_count):
        rows_here = board[place]
        for other_x in range(1, x_count):
            rows_here += board[other_x * y_count + place]
        grid[place * rows : (place + 1) * rows] = rows_here

    adjacency_copy.wait()
    whole = grid[...]
    row_id = lax.broadcasted_iota(jnp.int32, (grid_rows, lanes), 0)
    lane_id = lax.broadcasted_iota(jnp.int32, (grid_rows, lanes), 1)

    def quantity(number, link, keep):
        values = whole if number == 0 else pltpu.roll(whole, lanes - number * grid_columns, 1)
        return jnp.where(keep, values, 0.0)

    def widened(index):
        flat = adjacency_ref[index]
        if lanes > grid_columns:
            blank = jnp.zeros((grid_rows, lanes - grid_columns), jnp.int32)
            flat = jnp.concatenate([flat, blank], axis=1)
        return flat

    keep_down = (widened(1) > 0) & (row_id < grid_rows - 1) & (lane_id < grid_columns)
    keep_right = (widened(0) > 0) & (lane_id < grid_columns - 1)
    down_conf = quantity(0, 1, keep_down)
    down_off = quantity(1, 1, keep_down)
    right_conf = quantity(2, 0, keep_right)
    right_off = quantity(3, 0, keep_right)
    up_conf, up_off = pltpu.roll(down_conf, 1, 0), -pltpu.roll(down_off, 1, 0)
    left_conf, left_off = pltpu.roll(right_conf, 1, 1), -pltpu.roll(right_off, 1, 1)
    confidence_sum = up_conf + down_conf + left_conf + right_conf
    denominator = anchor_weight + confidence_sum
    push = (
        up_conf * up_off + down_conf * down_off + left_conf * left_off + right_conf * right_off
    ) / denominator
    up_part, down_part = up_conf / denominator, down_conf / denominator
    left_part, right_part = left_conf / denominator, right_conf / denominator
    pull = confidence_sum / denominator
    tiles = grid_rows * grid_columns

    def mean_of(values):
        return jnp.sum(jnp.sum(values, axis=0, keepdims=True), axis=1, keepdims=True) / tiles

    column_sums = (
        pltpu.roll(up_part, grid_rows - 1, 0) + pltpu.roll(down_part, 1, 0)
        + pltpu.roll(left_part, lanes - 1, 1) + pltpu.roll(right_part, 1, 1)
    )
    push_mean, pull_mean = mean_of(push), mean_of(pull)
    fresh, mean = push, push_mean
    for _ in range(ITERS - 1):
        ahead = mean_of(column_sums * fresh)
        fresh = (
            up_part * pltpu.roll(fresh, 1, 0)
            + down_part * pltpu.roll(fresh, grid_rows - 1, 0)
            + left_part * pltpu.roll(fresh, 1, 1)
            + right_part * pltpu.roll(fresh, lanes - 1, 1)
            + push
        ) - pull * mean
        mean = ahead + push_mean - pull_mean * mean
    log_gain = fresh - mean_of(fresh)
    result = jnp.zeros((rows, columns), jnp.float32)
    out_row = lax.broadcasted_iota(jnp.int32, (rows, columns), 0)
    out_column = lax.broadcasted_iota(jnp.int32, (rows, columns), 1)
    for row in range(rows):
        line = jnp.sum(jnp.where(row_id == y_index * rows + row, log_gain, 0.0), axis=0, keepdims=True)
        for column in range(columns):
            value = jnp.sum(
                jnp.where(lane_id[:1] == x_index * columns + column, line, 0.0), axis=1, keepdims=True
            )
            result += jnp.where((out_row == row) & (out_column == column), value, 0.0)
    out_ref[...] = result


def body(pixels, weights, adjacency):
    rows, columns, sides, length = pixels.shape
    steps = length // 128
    chunks = chunk_count(steps)
    x_count, y_count = lax.axis_size("gx"), lax.axis_size("gy")
    devices = x_count * y_count
    lanes = -(-4 * x_count * columns // 128) * 128

    def stacked(array):
        array = array.reshape(rows, columns, sides, steps, 128)
        return array.transpose(0, 1, 3, 2, 4).reshape(rows, columns, steps * sides, 128)

    def halo(count):
        return pltpu.VMEM((steps * count, 128), jnp.bfloat16)

    halos = [halo(columns), halo(columns), halo(rows), halo(rows)]
    return pl.pallas_call(
        functools.partial(kernel, (rows, columns, steps), chunks),
        in_specs=[pl.BlockSpec(memory_space=pl.ANY)] * 3,
        out_specs=pl.BlockSpec(memory_space=pltpu.VMEM),
        out_shape=pltpu.VMEM((rows, columns), jnp.float32),
        scratch_shapes=[
            pltpu.VMEM((rows, columns, steps * sides, 128), jnp.int32),
            pltpu.VMEM((rows, columns, steps * sides, 128), jnp.bfloat16),
            *halos,
            *halos,
            pltpu.VMEM((2 * len(all_groups(rows, columns)), 256, 256), jnp.float32),
            pltpu.VMEM((rows * columns * sides, 16, 16), jnp.float32),
            *([pltpu.VMEM((columns, 16, 16), jnp.float32), pltpu.VMEM((rows, 16, 16), jnp.float32)] * 2),
            pltpu.VMEM((rows, lanes), jnp.float32),
            pltpu.VMEM((devices, rows, lanes), jnp.float32),
            pltpu.VMEM((y_count * rows, lanes), jnp.float32),
            pltpu.VMEM(adjacency.shape, jnp.int32),
            pltpu.SemaphoreType.DMA((chunks,)),
            pltpu.SemaphoreType.DMA((chunks,)),
            pltpu.SemaphoreType.DMA((4,)),
            pltpu.SemaphoreType.DMA((4, chunks)),
            pltpu.SemaphoreType.DMA((2,)),
            pltpu.SemaphoreType.DMA((2,)),
            pltpu.SemaphoreType.DMA,
            pltpu.SemaphoreType.DMA,
            pltpu.SemaphoreType.DMA,
            halo(columns),
            pltpu.SemaphoreType.DMA((chunks,)),
            pltpu.SemaphoreType.DMA((chunks,)),
            pltpu.SemaphoreType.REGULAR((4,)),
        ],
        compiler_params=pltpu.CompilerParams(
            collective_id=0, has_side_effects=True, vmem_limit_bytes=60 * 1024 * 1024
        ),
        name="equalise",
    )(stacked(pixels), stacked(weights), adjacency)


def solution(mesh):
    return jax.shard_map(
        body,
        mesh=mesh,
        in_specs=(P("gy", "gx", None, None), P("gy", "gx", None, None), P()),
        out_specs=P("gy", "gx"),
        check_vma=False,
    )
```
